128 devices in a mesh: gx: 8 (over z_lo, y), gy: 16 (over z_hi, x, core).
Axes of the slice: x: 4, y: 4, z: 4 (z_hi: 2, z_lo: 2; z = z_hi * 2 + z_lo), core: 2. Of those that a mesh axis runs over, the one named last changes fastest.
Arguments:
- u_wind: float32 [60, 512, 2048], P(None, 'gx', 'gy'), may hold values from -6 to 6
- v_wind: float32 [60, 512, 2048], P(None, 'gx', 'gy'), may hold values from -6 to 6
- w_wind: float32 [60, 512, 2048], P(None, 'gx', 'gy'), may hold values from -3 to 3
- pressure: float32 [60, 512, 2048], P(None, 'gx', 'gy'), may hold values from -6 to 6
- vert_coef: float32 [512, 2048], P('gx', 'gy'), may hold values from 0.2 to 5
- we_slab: float32 [2, 3, 60, 5, 2048], P(None, None, None, None, ('gy', 'gx')), may hold values from -8 to 8
- sn_slab: float32 [2, 3, 60, 5, 512], P(None, None, None, None, ('gx', 'gy')), may hold values from -8 to 8
- relax_width: int32 [512, 2048], P('gx', 'gy'), may hold values from 2 to 5
Outputs:
- u_out: float32 [60, 512, 2048], P(None, 'gx', 'gy')
- v_out: float32 [60, 512, 2048], P(None, 'gx', 'gy')
- w_out: float32 [60, 512, 2048], P(None, 'gx', 'gy')
- p_out: float32 [60, 512, 2048], P(None, 'gx', 'gy')
The draws below stay inside these ranges and needn't reach their ends.
All inputs are finite; a program needn't handle non-finite values.
Results may differ from the reference program's by a relative error of at most 0.0001.
Values sent between devices are 32-bit elements; how exact they have to be, the bound alone decides.
A program may use at most 192 MiB of HBM per device.

```python
import math
import jax
import jax.numpy as jnp
from jax import lax

NZ = 60
W = 5
SUBSTEPS = 6
NX = 512
NY = 2048


def place_ends(drawn, stream_key, smallest, largest):
    shape = drawn.shape
    place = [jax.random.randint(jax.random.fold_in(stream_key, axis), (), 0, shape[axis]) for axis in range(len(shape))]
    drawn = drawn.at[tuple(place)].set(smallest)
    longest = shape.index(max(shape))
    place[longest] = (place[longest] + 1) % shape[longest]
    return drawn.at[tuple(place)].set(largest)


def level_of(rng, shape, split, smallest, high):
    level = 1.0
    for position, blocks in split:
        draws = jax.random.uniform(jax.random.fold_in(jax.random.fold_in(rng, 6), position), (blocks,), jnp.float32, smallest / len(split), high / len(split))
        level = level * jnp.repeat(jnp.exp(draws), shape[position] // blocks).reshape((-1,) + (1,) * (len(shape) - 1 - position))
    return level


def normal_values(own_key, dims, deviation, bound, pieces=(), kind=jnp.bfloat16):
    array = deviation * jax.random.normal(own_key, dims, jnp.float32)
    if pieces:
        array = array * level_of(own_key, dims, pieces, -0.22, 0.18)
    return jnp.clip(array, -bound, bound).astype(kind)


def setup_inputs(seed: int = 0) -> dict:
    seeds = jax.random.split(jax.random.key(seed), 9)
    u_wind = normal_values(seeds[0], (NZ, NX, NY), 1.0, 6.0, ((1, 8), (2, 16)), jnp.float32)
    v_wind = normal_values(seeds[1], (NZ, NX, NY), 1.0, 6.0, ((1, 8), (2, 16)), jnp.float32)
    w_wind = normal_values(seeds[2], (NZ, NX, NY), 0.5, 3.0, ((1, 8), (2, 16)), jnp.float32)
    pressure = normal_values(seeds[3], (NZ, NX, NY), 1.0, 6.0, ((1, 8), (2, 16)), jnp.float32)
    vert_coef = jnp.clip(jnp.exp(math.log(5.0) - 3.218876 * jax.random.uniform(seeds[4], (NX, NY), jnp.float32) ** level_of(seeds[4], (NX, NY), ((0, 8), (1, 16)), -0.2, 0.2)), 0.2, 5.0)
    we_slab = normal_values(seeds[5], (2, 3, NZ, W, NY), 1.5, 8.0, ((4, 128),), jnp.float32)
    sn_slab = normal_values(seeds[6], (2, 3, NZ, W, NX), 1.5, 8.0, ((4, 128),), jnp.float32)
    relax_width = place_ends(jax.random.randint(seeds[7], (NX, NY), 2, W + 1), jax.random.fold_in(seeds[7], 1), 2, W).astype(jnp.int32)
    return dict(u_wind=u_wind, v_wind=v_wind, w_wind=w_wind, pressure=pressure, vert_coef=vert_coef, we_slab=we_slab, sn_slab=sn_slab, relax_width=relax_width)


accel = 0.3
spread = 0.3
buoyancy = 0.5


def tri_solve(coef, rhs):
    def forward(carry, item):
        prev_c, prev_d = carry
        denom = 1.0 + 2.0 * coef + coef * prev_c
        next_c = -coef / denom
        next_d = (item + coef * prev_d) / denom
        return (next_c, next_d), (next_c, next_d)

    zero = jnp.zeros_like(coef)
    _, (cees, dees) = lax.scan(forward, (zero, zero), rhs)

    def backward(above, item):
        c_here, d_here = item
        value = d_here - c_here * above
        return value, value

    _, solved = lax.scan(backward, zero, (cees, dees), reverse=True)
    return solved


def blend(field, rows_k, cols_k, xpos, ypos, nx_total, ny_total, rate):
    band = rows_k.shape[2]
    size_x = field.shape[1]
    size_y = field.shape[2]
    west = jnp.pad(rows_k[0], ((0, 0), (0, size_x - band), (0, 0)))
    east = jnp.pad(rows_k[1][:, ::-1, :], ((0, 0), (size_x - band, 0), (0, 0)))
    south = jnp.pad(jnp.transpose(cols_k[0], (0, 2, 1)), ((0, 0), (0, 0), (0, size_y - band)))
    north = jnp.pad(jnp.transpose(cols_k[1][:, ::-1, :], (0, 2, 1)), ((0, 0), (0, 0), (size_y - band, 0)))
    weight_w = jnp.maximum(rate - xpos[:, None], 0.0) / rate
    weight_e = jnp.maximum(rate - (nx_total - 1.0 - xpos)[:, None], 0.0) / rate
    weight_s = jnp.maximum(rate - ypos[None, :], 0.0) / rate
    weight_n = jnp.maximum(rate - (ny_total - 1.0 - ypos)[None, :], 0.0) / rate
    field = field + weight_w[None] * (west - field)
    field = field + weight_e[None] * (east - field)
    field = field + weight_s[None] * (south - field)
    field = field + weight_n[None] * (north - field)
    return field


def column_part(u_new, v_new, west_u, south_v, w_old, p_old, coef):
    diverge = (u_new - west_u) + (v_new - south_v)
    sectioned = p_old - spread * diverge
    above_q = jnp.concatenate([sectioned[1:], jnp.zeros_like(sectioned[:1])], axis=0)
    rhs = w_old + buoyancy * (sectioned - above_q)
    w_new = tri_solve(coef, rhs)
    below_w = jnp.concatenate([jnp.zeros_like(w_new[:1]), w_new[:-1]], axis=0)
    p_new = sectioned - buoyancy * (w_new - below_w)
    return w_new, p_new


def reference(u_wind, v_wind, w_wind, pressure, vert_coef, we_slab, sn_slab, relax_width):
    size_x = pressure.shape[1]
    size_y = pressure.shape[2]
    xpos = jnp.arange(size_x, dtype=jnp.int32).astype(jnp.float32)
    ypos = jnp.arange(size_y, dtype=jnp.int32).astype(jnp.float32)
    rate = relax_width.astype(jnp.float32)
    fields = []
    for index, field in enumerate((u_wind, v_wind, pressure)):
        fields.append(blend(field, we_slab[:, index], sn_slab[:, index], xpos, ypos, float(size_x), float(size_y), rate))
    u_now, v_now, p_now = fields
    w_now = w_wind
    for step in range(SUBSTEPS):
        east_p = jnp.concatenate([p_now[:, 1:, :], jnp.zeros_like(p_now[:, :1, :])], axis=1)
        north_p = jnp.concatenate([p_now[:, :, 1:], jnp.zeros_like(p_now[:, :, :1])], axis=2)
        u_now = u_now - accel * (east_p - p_now)
        v_now = v_now - accel * (north_p - p_now)
        west_u = jnp.concatenate([jnp.zeros_like(u_now[:, :1, :]), u_now[:, :-1, :]], axis=1)
        south_v = jnp.concatenate([jnp.zeros_like(v_now[:, :, :1]), v_now[:, :, :-1]], axis=2)
        w_now, p_now = column_part(u_now, v_now, west_u, south_v, w_now, p_now, vert_coef)
    return u_now, v_now, w_now, p_now
```

```python
import functools

import jax
import jax.numpy as jnp
from jax import lax
from jax.experimental import pallas as pl
from jax.experimental.pallas import tpu as pltpu
from jax.sharding import PartitionSpec as PS

MESH = pl.DeviceIdType.MESH
STEPS = 6
GROUPS = 4
ORDER = (0, 3, 1, 2)
BAND = 5
F32 = jnp.float32


def kernel(ngx, ngy, nz, rx, ly,
           u_hbm, v_hbm, w_hbm, p_hbm, r_hbm, we_hbm, sn_hbm, rate_hbm,
           uo_hbm, vo_hbm, wo_hbm, po_hbm,
           P, E, S, W, G, U, V, R, RW, WEL, SNL, WPK, SPK, WEB, SNB, TT, BB, QQ,
           EB, RN, RS, EV, RV, SN, KK,
           lsem, osem, ssem, rsem, wssem, wrsem, sssem, srsem):
    gx = lax.axis_index("gx")
    gy = lax.axis_index("gy")
    rows = rx // GROUPS
    sy = ly // ngx
    sx = rx // ngy

    def load(i, src, dst):
        c = pltpu.make_async_copy(src, dst, lsem.at[i])
        c.start()
        return c

    l_we = load(5, we_hbm, WEL)
    l_sn = load(6, sn_hbm, SNL)
    l_r = load(4, r_hbm, R)
    l_rate = load(7, rate_hbm, RW)
    l_p = load(3, p_hbm, P.at[0, :, pl.ds(8, rx), :])
    l_u = load(0, u_hbm, U.at[:, pl.ds(8, rx), :])
    l_v = load(1, v_hbm, V)
    l_w = load(2, w_hbm, W)

    barrier = pltpu.get_barrier_semaphore()

    def peers(me, other, n):
        return (other != me) & (
            (other == me - 1) | (other == me + 1) | (other == 0) | (other == n - 1)
            | (me == 0) | (me == n - 1))

    count = jnp.int32(0)
    for k in range(ngx):
        ok = peers(gx, k, ngx)
        count = count + jnp.where(ok, 1, 0)

        @pl.when(ok)
        def _(k=k):
            pl.semaphore_signal(barrier, inc=1, device_id=(k, gy), device_id_type=MESH)
    for k in range(ngy):
        ok = peers(gy, k, ngy)
        count = count + jnp.where(ok, 1, 0)

        @pl.when(ok)
        def _(k=k):
            pl.semaphore_signal(barrier, inc=1, device_id=(gx, k), device_id_type=MESH)

    WPK[...] = jnp.zeros_like(WPK)
    SPK[...] = jnp.zeros_like(SPK)
    l_we.wait()
    l_sn.wait()
    for side in range(2):
        for i in range(3 * BAND):
            f, d = i // BAND, i % BAND
            lo = 0 if i < 8 else 64
            WPK[side, i % 8, :, lo:lo + nz] = WEL[side, f, d]
            SPK[side, i % 8, :, lo:lo + nz] = SNL[side, f, d]

    pl.semaphore_wait(barrier, count)

    def we_copy(side, k):
        dest = 0 if side == 0 else ngx - 1
        return pltpu.make_async_remote_copy(
            src_ref=WPK.at[side], dst_ref=WEB.at[k], send_sem=wssem.at[side],
            recv_sem=wrsem.at[k], device_id=(dest, gy), device_id_type=MESH)

    def sn_copy(side, k):
        dest = 0 if side == 0 else ngy - 1
        return pltpu.make_async_remote_copy(
            src_ref=SPK.at[side], dst_ref=SNB.at[k], send_sem=sssem.at[side],
            recv_sem=srsem.at[k], device_id=(gx, dest), device_id_type=MESH)

    for side in range(2):
        @pl.when(gx != (0 if side == 0 else ngx - 1))
        def _(side=side):
            we_copy(side, gx).start()

        @pl.when(gy != (0 if side == 0 else ngy - 1))
        def _(side=side):
            sn_copy(side, gy).start()

    l_r.wait()
    r_all = R[...]
    base = 1.0 + 2.0 * r_all

    def factor(z, prev):
        g = r_all / (base - r_all * prev)
        G[z] = g
        return g

    lax.fori_loop(0, nz, factor, jnp.zeros_like(r_all))

    l_rate.wait()
    l_p.wait()
    l_u.wait()
    l_v.wait()

    def field_row(f, x):
        if f == 0:
            return U.at[:, 8 + x, :]
        if f == 1:
            return V.at[:, x, :]
        return P.at[0, :, 8 + x, :]

    def blend_x(side):
        me = 0 if side == 0 else ngx - 1
        for k in range(ngx):
            if k == me:
                WEB[k] = WPK[side]
            else:
                we_copy(side, k).wait_recv()
        for i in range(8):
            for k in range(ngx):
                TT[k * sy:(k + 1) * sy, :] = WEB[k, i]
            turned = jnp.transpose(TT[...])
            for half in range(2):
                n = i + 8 * half
                if n >= 3 * BAND:
                    continue
                f, d = n // BAND, n % BAND
                x = d if side == 0 else rx - 1 - d
                rate = RW[x:x + 1, :].astype(F32)
                weight = jnp.maximum(rate - float(d), 0.0) / rate
                slab = turned[64 * half:64 * half + nz]
                row = field_row(f, x)
                old = row[...]
                row[...] = old + weight * (slab - old)

    def blend_y(side):
        me = 0 if side == 0 else ngy - 1
        for k in range(ngy):
            if k == me:
                SNB[k] = SPK[side]
            else:
                sn_copy(side, k).wait_recv()
        BB[...] = jnp.zeros_like(BB)
        TT[...] = jnp.zeros_like(TT)
        for i in range(8):
            for k in range(ngy):
                TT[k * sx:(k + 1) * sx, :] = SNB[k, i]
            turned = jnp.transpose(TT[...])
            for half in range(2):
                n = i + 8 * half
                if n >= 3 * BAND:
                    continue
                f, d = n // BAND, n % BAND
                dd = d if side == 0 else 7 - d
                BB[f, :, dd, :] = turned[64 * half:64 * half + 64]
        for f in range(3):
            for q in range(4):
                block = BB[f, 16 * q:16 * q + 16].reshape(128, 128)
                QQ[f, q] = jnp.transpose(block)[:rx]
        lane = lax.broadcasted_iota(jnp.int32, (rx, ly), 1).astype(F32)
        dist = lane if side == 0 else (ly - 1.0) - lane
        rate = RW[...].astype(F32)
        weight = jnp.maximum(rate - dist, 0.0) / rate

        def level(z, _):
            q = z // 16
            shift = (0 if side == 0 else 120) + 128 - 8 * (z % 16)
            shift = lax.rem(shift, 128)
            for f in range(3):
                slab = pltpu.roll(QQ[f, q], shift, 1)
                if f == 0:
                    dst = U.at[z, pl.ds(8, rx), :]
                elif f == 1:
                    dst = V.at[z]
                else:
                    dst = P.at[0, z, pl.ds(8, rx), :]
                old = dst[...]
                dst[...] = old + weight * (slab - old)
            return 0

        lax.fori_loop(0, nz, level, 0)

    for side in range(2):
        @pl.when(gx == (0 if side == 0 else ngx - 1))
        def _(side=side):
            blend_x(side)
    for side in range(2):
        @pl.when(gy == (0 if side == 0 else ngy - 1))
        def _(side=side):
            blend_y(side)

    pair = lax.broadcasted_iota(jnp.int32, (rows, ly), 1) // 2
    lane_r = lax.broadcasted_iota(jnp.int32, (rows, ly), 1)
    rim = (lane_r == 0) | (lane_r == ly - 1)

    def put(acc, value, z):
        return jnp.where(pair == z, pltpu.roll(value, lax.rem(2 * z + 1, 128), 1), acc)

    def own_rows(g):
        return pl.ds(8 + g * rows, rows)

    def all_rows(g):
        return pl.ds(g * rows, rows)

    def x_west(par):
        return pltpu.make_async_remote_copy(
            src_ref=P.at[par, :, pl.ds(8, 1), :], dst_ref=P.at[par, :, pl.ds(8 + rx, 1), :],
            send_sem=ssem.at[0, par], recv_sem=rsem.at[0, par],
            device_id=(gx - 1, gy), device_id_type=MESH)

    def x_east(par):
        return pltpu.make_async_remote_copy(
            src_ref=P.at[par, :, pl.ds(7 + rx, 1), :], dst_ref=P.at[par, :, pl.ds(7, 1), :],
            send_sem=ssem.at[1, par], recv_sem=rsem.at[1, par],
            device_id=(gx + 1, gy), device_id_type=MESH)

    def u_east():
        return pltpu.make_async_remote_copy(
            src_ref=U.at[:, pl.ds(7 + rx, 1), :], dst_ref=U.at[:, pl.ds(7, 1), :],
            send_sem=ssem.at[10, 0], recv_sem=rsem.at[10, 0],
            device_id=(gx + 1, gy), device_id_type=MESH)

    def y_north(par, g):
        return pltpu.make_async_remote_copy(
            src_ref=EB.at[par, all_rows(g)], dst_ref=RS.at[par, all_rows(g)],
            send_sem=ssem.at[2 + g, par], recv_sem=rsem.at[2 + g, par],
            device_id=(gx, gy + 1), device_id_type=MESH)

    def y_south(par, g):
        return pltpu.make_async_remote_copy(
            src_ref=EB.at[par, all_rows(g)], dst_ref=RN.at[par, all_rows(g)],
            send_sem=ssem.at[6 + g, par], recv_sem=rsem.at[6 + g, par],
            device_id=(gx, gy - 1), device_id_type=MESH)

    def v_north():
        return pltpu.make_async_remote_copy(
            src_ref=EV, dst_ref=RV,
            send_sem=ssem.at[11, 0], recv_sem=rsem.at[11, 0],
            device_id=(gx, gy + 1), device_id_type=MESH)

    has_w, has_e = gx > 0, gx < ngx - 1
    has_s, has_n = gy > 0, gy < ngy - 1

    def send_group(par, g):
        if g == 0:
            @pl.when(has_w)
            def _():
                x_west(par).start()

            @pl.when(jnp.logical_not(has_w))
            def _():
                P[par, :, 7, :] = P[par, :, 8, :]
        if g == GROUPS - 1:
            @pl.when(has_e)
            def _():
                x_east(par).start()

        @pl.when(has_n)
        def _():
            y_north(par, g).start()

        @pl.when(has_s)
        def _():
            y_south(par, g).start()

    def wait_group(par, g):
        if g == 0:
            @pl.when(has_w)
            def _():
                x_east(par).wait_recv()
                x_west(par).wait_send()
        if g == GROUPS - 1:
            @pl.when(has_e)
            def _():
                x_west(par).wait_recv()
                x_east(par).wait_send()

        @pl.when(has_n)
        def _():
            y_south(par, g).wait_recv()
            y_north(par, g).wait_send()

        @pl.when(has_s)
        def _():
            y_north(par, g).wait_recv()
            y_south(par, g).wait_send()

    @pl.when(jnp.logical_not(has_w))
    def _():
        U[:, 7, :] = jnp.zeros((nz, ly), F32)

    @pl.when(jnp.logical_not(has_e))
    def _():
        for par in range(2):
            P[par, :, 8 + rx, :] = jnp.zeros((nz, ly), F32)

    @pl.when(jnp.logical_not(has_n))
    def _():
        RN[...] = jnp.zeros_like(RN)

    @pl.when(jnp.logical_not(has_s))
    def _():
        RV[...] = jnp.zeros_like(RV)

    @pl.when(has_e)
    def _():
        u_east().start()

    for g in ORDER:
        def first(z, accs):
            acc_p, acc_v = accs
            return (put(acc_p, P[0, z, own_rows(g)], z), put(acc_v, V[z, all_rows(g)], z))

        none = jnp.zeros((rows, ly), F32)
        acc_p, acc_v = lax.fori_loop(0, nz, first, (none, none))
        EB[0, all_rows(g)] = acc_p
        EV[all_rows(g)] = acc_v
        send_group(0, g)

    @pl.when(has_n)
    def _():
        v_north().start()

    @pl.when(has_e)
    def _():
        u_east().wait_send()

    @pl.when(has_w)
    def _():
        u_east().wait_recv()

    @pl.when(has_n)
    def _():
        v_north().wait_send()

    @pl.when(has_s)
    def _():
        v_north().wait_recv()

    SN[...] = jnp.zeros_like(SN)
    S[:, rx, :] = jnp.zeros((nz, ly), F32)
    first_lane = lane_r == 0
    last_lane = lane_r == ly - 1
    for g in range(GROUPS):
        halo_v = RV[all_rows(g)]

        def divergence(z, _):
            u = U[z, own_rows(g)]
            uw = U[z, pl.ds(7 + g * rows, rows)]
            v = V[z, all_rows(g)]
            vs = jnp.where(first_lane, pltpu.roll(halo_v, lax.rem(128 - 2 * z, 128), 1),
                           pltpu.roll(v, 1, 1))
            E[z, all_rows(g)] = 0.3 * ((u - uw) + (v - vs))
            S[z, all_rows(g)] = jnp.zeros((rows, ly), F32)
            return 0

        lax.fori_loop(0, nz, divergence, 0)

    l_w.wait()

    even = lax.rem(lane_r, 2) == 0

    def corrections(cur, g):
        eb = EB[cur, all_rows(g)]
        rn = RN[cur, all_rows(g)]
        rs = jnp.where(has_s, RS[cur, all_rows(g)], pltpu.roll(eb, 127, 1))
        x = jnp.where(even, rs, rn) - eb
        SN[all_rows(g)] = SN[all_rows(g)] + rn
        return jnp.where(even, pltpu.roll(x, 127, 1), pltpu.roll(x, 1, 1))

    def forward(cur, nxt, g):
        r_rows = R[all_rows(g)]
        rinv = 1.0 / r_rows
        k_g = corrections(cur, g)

        def get_q(z):
            p = P[cur, z, own_rows(g)]
            pe = P[cur, z, pl.ds(9 + g * rows, rows)]
            pw = P[cur, z, pl.ds(7 + g * rows, rows)]
            ns = pltpu.roll(p, 1, 1) + pltpu.roll(p, 127, 1)
            k = jnp.where(rim, pltpu.roll(k_g, lax.rem(255 - 2 * z, 128), 1), 0.0)
            total = (pe + pw) + (ns + k)
            e = E[z, all_rows(g)] + 0.09 * (4.0 * p - total)
            E[z, all_rows(g)] = e
            S[z, all_rows(g)] = S[z, all_rows(g)] + p
            q = p - e
            P[nxt, z, own_rows(g)] = q
            return q

        def one(z, carry, last=False):
            q, dprev = carry
            if last:
                qn, diff = q, q
            else:
                qn = get_q(z + 1)
                diff = q - qn
            rhs = W[z, all_rows(g)] + 0.5 * diff
            d = G[z, all_rows(g)] * (rinv * rhs + dprev)
            W[z, all_rows(g)] = d
            return qn, d

        carry = (get_q(0), jnp.zeros((rows, ly), F32))
        unroll = 4
        head = (nz - 1) % unroll
        for z in range(head):
            carry = one(z, carry)

        def body(i, carry):
            for k in range(unroll):
                carry = one(head + i * unroll + k, carry)
            return carry

        carry = lax.fori_loop(0, (nz - 1) // unroll, body, carry)
        one(nz - 1, carry, last=True)

    def backward(nxt, g, edges):
        none = jnp.zeros((rows, ly), F32)

        def one(z, carry):
            w_up, h_up, acc = carry
            w = W[z, all_rows(g)] + G[z, all_rows(g)] * w_up
            W[z, all_rows(g)] = w
            h = 0.5 * w
            p = (P[nxt, z + 1, own_rows(g)] - h_up) + h
            P[nxt, z + 1, own_rows(g)] = p
            if edges:
                acc = put(acc, p, z + 1)
            return w, h, acc

        w_top = W[nz - 1, all_rows(g)]
        carry = (w_top, 0.5 * w_top, none)
        unroll = 4
        head = (nz - 1) % unroll
        for k in range(head):
            carry = one(nz - 2 - k, carry)

        def body(i, carry):
            for k in range(unroll):
                carry = one(nz - 2 - head - i * unroll - k, carry)
            return carry

        _, h_up, acc = lax.fori_loop(0, (nz - 1) // unroll, body, carry)
        p = P[nxt, 0, own_rows(g)] - h_up
        P[nxt, 0, own_rows(g)] = p
        if edges:
            EB[nxt, all_rows(g)] = put(acc, p, 0)

    def east_sum(cur):
        S[:, rx, :] = S[:, rx, :] + P[cur, :, 8 + rx, :]

    def step(s, _):
        cur = lax.rem(s, 2)
        nxt = 1 - cur
        for g in ORDER:
            wait_group(cur, g)
            if g == GROUPS - 1:
                east_sum(cur)
            forward(cur, nxt, g)
            backward(nxt, g, True)
            send_group(nxt, g)
        return 0

    lax.fori_loop(0, STEPS - 1, step, 0)

    cur = (STEPS - 1) % 2
    nxt = 1 - cur
    outs = []

    def store(i, src, dst):
        c = pltpu.make_async_copy(src, dst, osem.at[i])
        c.start()
        outs.append(c)

    for g in ORDER:
        wait_group(cur, g)
        if g == GROUPS - 1:
            east_sum(cur)
        forward(cur, nxt, g)
        backward(nxt, g, False)
        store(g, W.at[:, all_rows(g), :], wo_hbm.at[:, all_rows(g), :])
        store(4 + g, P.at[nxt, :, own_rows(g), :], po_hbm.at[:, all_rows(g), :])
    for g in range(GROUPS):
        halo = SN[all_rows(g)]

        def winds(z, _):
            t = S[z, all_rows(g)]
            te = S[z, pl.ds(g * rows + 1, rows)]
            tn = jnp.where(last_lane, pltpu.roll(halo, lax.rem(254 - 2 * z, 128), 1),
                           pltpu.roll(t, 127, 1))
            U[z, own_rows(g)] = U[z, own_rows(g)] - 0.3 * (te - t)
            V[z, all_rows(g)] = V[z, all_rows(g)] - 0.3 * (tn - t)
            return 0

        lax.fori_loop(0, nz, winds, 0)
        store(8 + g, U.at[:, own_rows(g), :], uo_hbm.at[:, all_rows(g), :])
        store(12 + g, V.at[:, all_rows(g), :], vo_hbm.at[:, all_rows(g), :])

    for side in range(2):
        @pl.when(gx != (0 if side == 0 else ngx - 1))
        def _(side=side):
            we_copy(side, gx).wait_send()

        @pl.when(gy != (0 if side == 0 else ngy - 1))
        def _(side=side):
            sn_copy(side, gy).wait_send()
    for c in outs:
        c.wait()


def per_device(ngx, ngy, u, v, w, p, r, we, sn, rate):
    nz, rx, ly = p.shape
    we = jnp.transpose(we, (0, 1, 3, 4, 2))
    sn = jnp.transpose(sn, (0, 1, 3, 4, 2))
    field = jax.ShapeDtypeStruct((nz, rx, ly), F32)
    vm = lambda *s: pltpu.VMEM(s, F32)
    any_ = pl.BlockSpec(memory_space=pl.ANY)
    dma = pltpu.SemaphoreType.DMA
    scratch = [
        vm(2, nz, rx + 16, ly), vm(nz, rx, ly), vm(nz, rx + 8, ly), vm(nz, rx, ly), vm(nz, rx, ly),
        vm(nz, rx + 8, ly), vm(nz, rx, ly), vm(rx, ly), pltpu.VMEM((rx, ly), jnp.int32),
        vm(2, 3, BAND, ly // ngx, nz), vm(2, 3, BAND, rx // ngy, nz),
        vm(2, 8, ly // ngx, 128), vm(2, 8, rx // ngy, 128),
        vm(ngx, 8, ly // ngx, 128), vm(ngy, 8, rx // ngy, 128),
        vm(128, 128), vm(3, 64, 8, 128), vm(3, 4, rx, 128),
        vm(2, rx, ly), vm(2, rx, ly), vm(2, rx, ly), vm(rx, ly), vm(rx, ly), vm(rx, ly), vm(rx, ly),
        dma((8,)), dma((16,)), dma((12, 2)), dma((12, 2)),
        dma((2,)), dma((ngx,)), dma((2,)), dma((ngy,)),
    ]
    return pl.pallas_call(
        functools.partial(kernel, ngx, ngy, nz, rx, ly),
        out_shape=(field,) * 4,
        in_specs=[any_] * 8,
        out_specs=(any_,) * 4,
        scratch_shapes=scratch,
        compiler_params=pltpu.CompilerParams(collective_id=0, has_side_effects=True,
                                             vmem_limit_bytes=48 * 1024 * 1024),
    )(u, v, w, p, r, we, sn, rate)


def solution(mesh):
    ngx, ngy = mesh.shape["gx"], mesh.shape["gy"]
    grid = PS(None, "gx", "gy")
    return jax.shard_map(
        functools.partial(per_device, ngx, ngy),
        mesh=mesh,
        in_specs=(grid,) * 4 + (
            PS("gx", "gy"),
            PS(None, None, None, None, ("gy", "gx")),
            PS(None, None, None, None, ("gx", "gy")),
            PS("gx", "gy"),
        ),
        out_specs=(grid,) * 4,
        check_vma=False,
    )
```

```python
import functools

import jax
import jax.numpy as jnp
from jax import lax
from jax.experimental import pallas as pl
from jax.experimental.pallas import tpu as pltpu
from jax.sharding import PartitionSpec as PS

MESH = pl.DeviceIdType.MESH
STEPS = 6
GROUPS = 4
BAND = 5
F32 = jnp.float32


def kernel(ngx, ngy, nz, rx, ly,
           u_hbm, v_hbm, w_hbm, p_hbm, r_hbm, we_hbm, sn_hbm, rate_hbm,
           uo_hbm, vo_hbm, wo_hbm, po_hbm,
           PA, PB, E, S, W, G, U, V, R, RW, WEL, SNL, WPK, SPK, WEB, SNB, TT, BB, QQ,
           EB, RN, RS, EV, RV, SN, KK,
           lsem, osem, ssem, rsem, wssem, wrsem, sssem, srsem):
    P = (PA, PB)
    gx = lax.axis_index("gx")
    gy = lax.axis_index("gy")
    rows = rx // GROUPS
    sy = ly // ngx
    sx = rx // ngy

    def load(i, src, dst):
        c = pltpu.make_async_copy(src, dst, lsem.at[i])
        c.start()
        return c

    l_we = load(5, we_hbm, WEL)
    l_sn = load(6, sn_hbm, SNL)
    l_r = load(4, r_hbm, R)
    l_rate = load(7, rate_hbm, RW)
    l_p = load(3, p_hbm, PA.at[:, pl.ds(8, rx), :])
    l_u = load(0, u_hbm, U.at[:, pl.ds(8, rx), :])
    l_v = load(1, v_hbm, V)
    l_w = load(2, w_hbm, W)

    barrier = pltpu.get_barrier_semaphore()

    def peers(me, other, n):
        return (other != me) & (
            (other == me - 1) | (other == me + 1) | (other == 0) | (other == n - 1)
            | (me == 0) | (me == n - 1))

    count = jnp.int32(0)
    for k in range(ngx):
        ok = peers(gx, k, ngx)
        count = count + jnp.where(ok, 1, 0)

        @pl.when(ok)
        def _(k=k):
            pl.semaphore_signal(barrier, inc=1, device_id=(k, gy), device_id_type=MESH)
    for k in range(ngy):
        ok = peers(gy, k, ngy)
        count = count + jnp.where(ok, 1, 0)

        @pl.when(ok)
        def _(k=k):
            pl.semaphore_signal(barrier, inc=1, device_id=(gx, k), device_id_type=MESH)

    WPK[...] = jnp.zeros_like(WPK)
    SPK[...] = jnp.zeros_like(SPK)
    l_we.wait()
    l_sn.wait()
    for side in range(2):
        for i in range(3 * BAND):
            f, d = i // BAND, i % BAND
            lo = 0 if i < 8 else 64
            WPK[side, i % 8, :, lo:lo + nz] = WEL[side, f, d]
            SPK[side, i % 8, :, lo:lo + nz] = SNL[side, f, d]

    pl.semaphore_wait(barrier, count)

    def we_copy(side, k):
        dest = 0 if side == 0 else ngx - 1
        return pltpu.make_async_remote_copy(
            src_ref=WPK.at[side], dst_ref=WEB.at[k], send_sem=wssem.at[side],
            recv_sem=wrsem.at[k], device_id=(dest, gy), device_id_type=MESH)

    def sn_copy(side, k):
        dest = 0 if side == 0 else ngy - 1
        return pltpu.make_async_remote_copy(
            src_ref=SPK.at[side], dst_ref=SNB.at[k], send_sem=sssem.at[side],
            recv_sem=srsem.at[k], device_id=(gx, dest), device_id_type=MESH)

    for side in range(2):
        @pl.when(gx != (0 if side == 0 else ngx - 1))
        def _(side=side):
            we_copy(side, gx).start()

        @pl.when(gy != (0 if side == 0 else ngy - 1))
        def _(side=side):
            sn_copy(side, gy).start()

    l_r.wait()
    r_all = R[...]
    base = 1.0 + 2.0 * r_all

    def factor(z, prev):
        g = r_all / (base - r_all * prev)
        G[z] = g
        return g

    lax.fori_loop(0, nz, factor, jnp.zeros_like(r_all))

    l_rate.wait()
    l_p.wait()
    l_u.wait()
    l_v.wait()

    def field_row(f, x):
        if f == 0:
            return U.at[:, 8 + x, :]
        if f == 1:
            return V.at[:, x, :]
        return PA.at[:, 8 + x, :]

    def blend_x(side):
        me = 0 if side == 0 else ngx - 1
        for k in range(ngx):
            if k == me:
                WEB[k] = WPK[side]
            else:
                we_copy(side, k).wait_recv()
        for i in range(8):
            for k in range(ngx):
                TT[k * sy:(k + 1) * sy, :] = WEB[k, i]
            turned = jnp.transpose(TT[...])
            for half in range(2):
                n = i + 8 * half
                if n >= 3 * BAND:
                    continue
                f, d = n // BAND, n % BAND
                x = d if side == 0 else rx - 1 - d
                rate = RW[x:x + 1, :].astype(F32)
                weight = jnp.maximum(rate - float(d), 0.0) / rate
                slab = turned[64 * half:64 * half + nz]
                row = field_row(f, x)
                old = row[...]
                row[...] = old + weight * (slab - old)

    def blend_y(side):
        me = 0 if side == 0 else ngy - 1
        for k in range(ngy):
            if k == me:
                SNB[k] = SPK[side]
            else:
                sn_copy(side, k).wait_recv()
        BB[...] = jnp.zeros_like(BB)
        TT[...] = jnp.zeros_like(TT)
        for i in range(8):
            for k in range(ngy):
                TT[k * sx:(k + 1) * sx, :] = SNB[k, i]
            turned = jnp.transpose(TT[...])
            for half in range(2):
                n = i + 8 * half
                if n >= 3 * BAND:
                    continue
                f, d = n // BAND, n % BAND
                dd = d if side == 0 else 7 - d
                BB[f, :, dd, :] = turned[64 * half:64 * half + 64]
        for f in range(3):
            for q in range(4):
                block = BB[f, 16 * q:16 * q + 16].reshape(128, 128)
                QQ[f, q] = jnp.transpose(block)[:rx]
        lane = lax.broadcasted_iota(jnp.int32, (rows, ly), 1).astype(F32)
        dist = lane if side == 0 else (ly - 1.0) - lane

        def part(g, _):
            at = pl.multiple_of(g * rows, 8)
            rate = RW[pl.ds(at, rows)].astype(F32)
            weight = jnp.maximum(rate - dist, 0.0) / rate
            for f in range(3):
                for z in range(nz):
                    shift = ((0 if side == 0 else 120) + 128 - 8 * (z % 16)) % 128
                    slab = pltpu.roll(QQ[f, z // 16, pl.ds(at, rows)], shift, 1)
                    if f == 0:
                        dst = U.at[z, pl.ds(at + 8, rows), :]
                    elif f == 1:
                        dst = V.at[z, pl.ds(at, rows), :]
                    else:
                        dst = PA.at[z, pl.ds(at + 8, rows), :]
                    old = dst[...]
                    dst[...] = old + weight * (slab - old)
            return 0

        lax.fori_loop(0, GROUPS, part, 0)

    for side in range(2):
        @pl.when(gx == (0 if side == 0 else ngx - 1))
        def _(side=side):
            blend_x(side)
    for side in range(2):
        @pl.when(gy == (0 if side == 0 else ngy - 1))
        def _(side=side):
            blend_y(side)

    pair = lax.broadcasted_iota(jnp.int32, (rows, ly), 1) // 2
    lane_r = lax.broadcasted_iota(jnp.int32, (rows, ly), 1)
    rim = (lane_r == 0) | (lane_r == ly - 1)

    def put(acc, value, z):
        return jnp.where(pair == z, pltpu.roll(value, (2 * z + 1) % 128, 1), acc)

    def own_rows(g):
        return pl.ds(pl.multiple_of(8 + g * rows, 8), rows)

    def all_rows(g):
        return pl.ds(pl.multiple_of(g * rows, 8), rows)

    def in_order(i):
        return jnp.where(i == 0, 0, jnp.where(i == 1, GROUPS - 1, i - 1))

    def x_west(par):
        return pltpu.make_async_remote_copy(
            src_ref=P[par].at[:, pl.ds(8, 1), :], dst_ref=P[par].at[:, pl.ds(8 + rx, 1), :],
            send_sem=ssem.at[0, par], recv_sem=rsem.at[0, par],
            device_id=(gx - 1, gy), device_id_type=MESH)

    def x_east(par):
        return pltpu.make_async_remote_copy(
            src_ref=P[par].at[:, pl.ds(7 + rx, 1), :], dst_ref=P[par].at[:, pl.ds(7, 1), :],
            send_sem=ssem.at[1, par], recv_sem=rsem.at[1, par],
            device_id=(gx + 1, gy), device_id_type=MESH)

    def u_east():
        return pltpu.make_async_remote_copy(
            src_ref=U.at[:, pl.ds(7 + rx, 1), :], dst_ref=U.at[:, pl.ds(7, 1), :],
            send_sem=ssem.at[10, 0], recv_sem=rsem.at[10, 0],
            device_id=(gx + 1, gy), device_id_type=MESH)

    def y_north(par, g):
        return pltpu.make_async_remote_copy(
            src_ref=EB.at[par, all_rows(g)], dst_ref=RS.at[par, all_rows(g)],
            send_sem=ssem.at[2 + g, par], recv_sem=rsem.at[2 + g, par],
            device_id=(gx, gy + 1), device_id_type=MESH)

    def y_south(par, g):
        return pltpu.make_async_remote_copy(
            src_ref=EB.at[par, all_rows(g)], dst_ref=RN.at[par, all_rows(g)],
            send_sem=ssem.at[6 + g, par], recv_sem=rsem.at[6 + g, par],
            device_id=(gx, gy - 1), device_id_type=MESH)

    def v_north():
        return pltpu.make_async_remote_copy(
            src_ref=EV, dst_ref=RV,
            send_sem=ssem.at[11, 0], recv_sem=rsem.at[11, 0],
            device_id=(gx, gy + 1), device_id_type=MESH)

    has_w, has_e = gx > 0, gx < ngx - 1
    has_s, has_n = gy > 0, gy < ngy - 1

    def send_group(par, g):
        @pl.when((g == 0) & has_w)
        def _():
            x_west(par).start()

        @pl.when((g == 0) & jnp.logical_not(has_w))
        def _():
            P[par][:, 7, :] = P[par][:, 8, :]

        @pl.when((g == GROUPS - 1) & has_e)
        def _():
            x_east(par).start()

        @pl.when(has_n)
        def _():
            y_north(par, g).start()

        @pl.when(has_s)
        def _():
            y_south(par, g).start()

    def wait_group(par, g):
        @pl.when((g == 0) & has_w)
        def _():
            x_east(par).wait_recv()
            x_west(par).wait_send()

        @pl.when((g == GROUPS - 1) & has_e)
        def _():
            x_west(par).wait_recv()
            x_east(par).wait_send()

        @pl.when(g == GROUPS - 1)
        def _():
            S[:, rx, :] = S[:, rx, :] + P[par][:, 8 + rx, :]

        @pl.when(has_n)
        def _():
            y_south(par, g).wait_recv()
            y_north(par, g).wait_send()

        @pl.when(has_s)
        def _():
            y_north(par, g).wait_recv()
            y_south(par, g).wait_send()

    @pl.when(jnp.logical_not(has_w))
    def _():
        U[:, 7, :] = jnp.zeros((nz, ly), F32)

    @pl.when(jnp.logical_not(has_e))
    def _():
        for par in range(2):
            P[par][:, 8 + rx, :] = jnp.zeros((nz, ly), F32)

    @pl.when(jnp.logical_not(has_n))
    def _():
        RN[...] = jnp.zeros_like(RN)

    @pl.when(jnp.logical_not(has_s))
    def _():
        RV[...] = jnp.zeros_like(RV)

    @pl.when(has_e)
    def _():
        u_east().start()

    def first(i, _):
        g = in_order(i)
        acc_p = jnp.zeros((rows, ly), F32)
        acc_v = jnp.zeros((rows, ly), F32)
        for z in range(nz):
            acc_p = put(acc_p, PA[z, own_rows(g)], z)
            acc_v = put(acc_v, V[z, all_rows(g)], z)
        EB[0, all_rows(g)] = acc_p
        EV[all_rows(g)] = acc_v
        send_group(0, g)
        return 0

    lax.fori_loop(0, GROUPS, first, 0)

    @pl.when(has_n)
    def _():
        v_north().start()

    @pl.when(has_e)
    def _():
        u_east().wait_send()

    @pl.when(has_w)
    def _():
        u_east().wait_recv()

    @pl.when(has_n)
    def _():
        v_north().wait_send()

    @pl.when(has_s)
    def _():
        v_north().wait_recv()

    SN[...] = jnp.zeros_like(SN)
    S[:, rx, :] = jnp.zeros((nz, ly), F32)
    first_lane = lane_r == 0
    last_lane = lane_r == ly - 1

    def divergence(g, _):
        halo_v = RV[all_rows(g)]
        for z in range(nz):
            u = U[z, own_rows(g)]
            uw = U[z, pl.ds(7 + g * rows, rows)]
            v = V[z, all_rows(g)]
            vs = jnp.where(first_lane, pltpu.roll(halo_v, (128 - 2 * z) % 128, 1),
                           pltpu.roll(v, 1, 1))
            E[z, all_rows(g)] = 0.3 * ((u - uw) + (v - vs))
            S[z, all_rows(g)] = jnp.zeros((rows, ly), F32)
        return 0

    lax.fori_loop(0, GROUPS, divergence, 0)

    l_w.wait()

    even = lax.rem(lane_r, 2) == 0

    def corrections(cur, g):
        eb = EB[cur, all_rows(g)]
        rn = RN[cur, all_rows(g)]
        rs = jnp.where(has_s, RS[cur, all_rows(g)], pltpu.roll(eb, 127, 1))
        x = jnp.where(even, rs, rn) - eb
        SN[all_rows(g)] = SN[all_rows(g)] + rn
        return jnp.where(even, pltpu.roll(x, 127, 1), pltpu.roll(x, 1, 1))

    def forward(cur, nxt, g):
        rinv = 1.0 / R[all_rows(g)]
        k_g = corrections(cur, g)

        def get_q(z):
            p = P[cur][z, own_rows(g)]
            pe = P[cur][z, pl.ds(9 + g * rows, rows)]
            pw = P[cur][z, pl.ds(7 + g * rows, rows)]
            ns = pltpu.roll(p, 1, 1) + pltpu.roll(p, 127, 1)
            k = jnp.where(rim, pltpu.roll(k_g, (255 - 2 * z) % 128, 1), 0.0)
            total = (pe + pw) + (ns + k)
            e = E[z, all_rows(g)] + 0.09 * (4.0 * p - total)
            E[z, all_rows(g)] = e
            S[z, all_rows(g)] = S[z, all_rows(g)] + p
            q = p - e
            P[nxt][z, own_rows(g)] = q
            return q

        q, d = get_q(0), jnp.zeros((rows, ly), F32)
        for z in range(nz):
            qn = get_q(z + 1) if z < nz - 1 else None
            diff = q - qn if z < nz - 1 else q
            rhs = W[z, all_rows(g)] + 0.5 * diff
            d = G[z, all_rows(g)] * (rinv * rhs + d)
            W[z, all_rows(g)] = d
            q = qn

    def backward(nxt, g, edges):
        acc = jnp.zeros((rows, ly), F32)
        w = W[nz - 1, all_rows(g)]
        h = 0.5 * w
        for z in range(nz - 2, -2, -1):
            p = P[nxt][z + 1, own_rows(g)] - h
            if z >= 0:
                w = W[z, all_rows(g)] + G[z, all_rows(g)] * w
                W[z, all_rows(g)] = w
                h = 0.5 * w
                p = p + h
            P[nxt][z + 1, own_rows(g)] = p
            if edges:
                acc = put(acc, p, z + 1)
        if edges:
            EB[nxt, all_rows(g)] = acc

    def step(cur, nxt):
        def part(i, _):
            g = in_order(i)
            wait_group(cur, g)
            forward(cur, nxt, g)
            backward(nxt, g, True)
            send_group(nxt, g)
            return 0

        lax.fori_loop(0, GROUPS, part, 0)

    def two_steps(i, _):
        step(0, 1)
        step(1, 0)
        return 0

    lax.fori_loop(0, (STEPS - 2) // 2, two_steps, 0)
    step(0, 1)

    def stores(g, which):
        to = lambda ref: ref.at[:, all_rows(g), :]
        pairs = ((W.at[:, all_rows(g), :], to(wo_hbm)), (PA.at[:, own_rows(g), :], to(po_hbm)),
                 (U.at[:, own_rows(g), :], to(uo_hbm)), (V.at[:, all_rows(g), :], to(vo_hbm)))
        return [pltpu.make_async_copy(*pairs[k], osem.at[k, g]) for k in which]

    def last(i, _):
        g = in_order(i)
        wait_group(1, g)
        forward(1, 0, g)
        backward(0, g, False)
        for c in stores(g, (0, 1)):
            c.start()
        return 0

    lax.fori_loop(0, GROUPS, last, 0)

    def winds(g, _):
        halo = SN[all_rows(g)]
        for z in range(nz):
            t = S[z, all_rows(g)]
            te = S[z, pl.ds(g * rows + 1, rows)]
            tn = jnp.where(last_lane, pltpu.roll(halo, (254 - 2 * z) % 128, 1),
                           pltpu.roll(t, 127, 1))
            U[z, own_rows(g)] = U[z, own_rows(g)] - 0.3 * (te - t)
            V[z, all_rows(g)] = V[z, all_rows(g)] - 0.3 * (tn - t)
        for c in stores(g, (2, 3)):
            c.start()
        return 0

    lax.fori_loop(0, GROUPS, winds, 0)

    for side in range(2):
        @pl.when(gx != (0 if side == 0 else ngx - 1))
        def _(side=side):
            we_copy(side, gx).wait_send()

        @pl.when(gy != (0 if side == 0 else ngy - 1))
        def _(side=side):
            sn_copy(side, gy).wait_send()
    for g in range(GROUPS):
        for c in stores(g, range(4)):
            c.wait()


def per_device(ngx, ngy, u, v, w, p, r, we, sn, rate):
    nz, rx, ly = p.shape
    we = jnp.transpose(we, (0, 1, 3, 4, 2))
    sn = jnp.transpose(sn, (0, 1, 3, 4, 2))
    field = jax.ShapeDtypeStruct((nz, rx, ly), F32)
    vm = lambda *s: pltpu.VMEM(s, F32)
    any_ = pl.BlockSpec(memory_space=pl.ANY)
    dma = pltpu.SemaphoreType.DMA
    scratch = [
        vm(nz, rx + 16, ly), vm(nz, rx + 16, ly), vm(nz, rx, ly), vm(nz, rx + 8, ly), vm(nz, rx, ly), vm(nz, rx, ly),
        vm(nz, rx + 8, ly), vm(nz, rx, ly), vm(rx, ly), pltpu.VMEM((rx, ly), jnp.int32),
        vm(2, 3, BAND, ly // ngx, nz), vm(2, 3, BAND, rx // ngy, nz),
        vm(2, 8, ly // ngx, 128), vm(2, 8, rx // ngy, 128),
        vm(ngx, 8, ly // ngx, 128), vm(ngy, 8, rx // ngy, 128),
        vm(128, 128), vm(3, 64, 8, 128), vm(3, 4, rx, 128),
        vm(2, rx, ly), vm(2, rx, ly), vm(2, rx, ly), vm(rx, ly), vm(rx, ly), vm(rx, ly), vm(rx, ly),
        dma((8,)), dma((4, GROUPS)), dma((12, 2)), dma((12, 2)),
        dma((2,)), dma((ngx,)), dma((2,)), dma((ngy,)),
    ]
    return pl.pallas_call(
        functools.partial(kernel, ngx, ngy, nz, rx, ly),
        out_shape=(field,) * 4,
        in_specs=[any_] * 8,
        out_specs=(any_,) * 4,
        scratch_shapes=scratch,
        compiler_params=pltpu.CompilerParams(collective_id=0, has_side_effects=True,
                                             vmem_limit_bytes=63 * 1024 * 1024),
    )(u, v, w, p, r, we, sn, rate)


def solution(mesh):
    ngx, ngy = mesh.shape["gx"], mesh.shape["gy"]
    grid = PS(None, "gx", "gy")
    return jax.shard_map(
        functools.partial(per_device, ngx, ngy),
        mesh=mesh,
        in_specs=(grid,) * 4 + (
            PS("gx", "gy"),
            PS(None, None, None, None, ("gy", "gx")),
            PS(None, None, None, None, ("gx", "gy")),
            PS("gx", "gy"),
        ),
        out_specs=(grid,) * 4,
        check_vma=False,
    )
```

```python
import functools

import jax
import jax.numpy as jnp
from jax import lax
from jax.experimental import pallas as pl
from jax.experimental.pallas import tpu as pltpu
from jax.sharding import PartitionSpec as PS

MESH = pl.DeviceIdType.MESH
STEPS = 6
GROUPS = 4
BAND = 5
F32 = jnp.float32


def kernel(ngx, ngy, nz, rx, ly,
           u_hbm, v_hbm, w_hbm, p_hbm, r_hbm, we_hbm, sn_hbm, rate_hbm,
           W, PA, U, V, S, SN,
           PB, E, G, R, RW, WEL, SNL, WPK, SPK, WEB, SNB, TT, BB, BN, QQ, FO,
           QX, EB, ES, RN, RS, EV, RV,
           lsem, ssem, rsem, wssem, wrsem, sssem, srsem):
    P = (PA, PB)
    gx = lax.axis_index("gx")
    gy = lax.axis_index("gy")
    has_w, has_e = gx > 0, gx < ngx - 1
    has_s, has_n = gy > 0, gy < ngy - 1
    rows = rx // GROUPS
    sy = ly // ngx
    sx = rx // ngy

    def load(i, src, dst):
        c = pltpu.make_async_copy(src, dst, lsem.at[i])
        c.start()
        return c

    l_we = load(5, we_hbm, WEL)
    l_sn = load(6, sn_hbm, SNL)
    l_r = load(4, r_hbm, R)
    l_rate = load(7, rate_hbm, RW)
    l_p = load(3, p_hbm, PA.at[:, pl.ds(8, rx), :])
    l_u = load(0, u_hbm, U.at[:, pl.ds(8, rx), :])
    l_v = load(1, v_hbm, V)
    l_w = load(2, w_hbm, W)

    barrier = pltpu.get_barrier_semaphore()

    def peers(me, other, n):
        return (other != me) & (
            (other == me - 1) | (other == me + 1) | (other == 0) | (other == n - 1)
            | (me == 0) | (me == n - 1))

    count = jnp.int32(0)
    for k in range(ngx):
        ok = peers(gx, k, ngx)
        count = count + jnp.where(ok, 1, 0)

        @pl.when(ok)
        def _(k=k):
            pl.semaphore_signal(barrier, inc=1, device_id=(k, gy), device_id_type=MESH)
    for k in range(ngy):
        ok = peers(gy, k, ngy)
        count = count + jnp.where(ok, 1, 0)

        @pl.when(ok)
        def _(k=k):
            pl.semaphore_signal(barrier, inc=1, device_id=(gx, k), device_id_type=MESH)

    WPK[...] = jnp.zeros_like(WPK)
    BB[...] = jnp.zeros_like(BB)
    BN[...] = jnp.zeros_like(BN)
    TT[...] = jnp.zeros_like(TT)
    l_we.wait()
    l_sn.wait()
    for side in range(2):
        for i in range(3 * BAND):
            f, d = i // BAND, i % BAND
            lo = 0 if i < 8 else 64
            WPK[side, i % 8, :, lo:lo + nz] = WEL[side, f, d]

    wide = 6 * sx
    per = 128 // wide
    for lot in range(0, BAND, per):
        for d in range(lot, min(lot + per, BAND)):
            for side in range(2):
                for f in range(3):
                    at = (d - lot) * wide + (side * 3 + f) * sx
                    TT[at:at + sx, 0:nz] = SNL[side, f, d]
        turned = jnp.transpose(TT[...])[:64]
        for d in range(lot, min(lot + per, BAND)):
            shift = (128 - (d - lot) * wide) % 128
            moved = pltpu.roll(turned, shift, 1) if shift else turned
            BB[:, d, :] = moved
            BN[:, 7 - d, :] = moved
    for q in range(4):
        for side, ref in enumerate((BB, BN)):
            block = jnp.transpose(ref[16 * q:16 * q + 16].reshape(128, 128))
            SPK[side, q * 3 * sx:(q + 1) * 3 * sx, :] = block[side * 3 * sx:(side + 1) * 3 * sx]

    l_r.wait()
    r_all = R[...]
    base = 1.0 + 2.0 * r_all

    def factor(z, prev):
        g = r_all / (base - r_all * prev)
        G[z] = g
        return g

    lax.fori_loop(0, nz, factor, jnp.zeros_like(r_all))

    pl.semaphore_wait(barrier, count)

    def we_copy(side, k):
        dest = 0 if side == 0 else ngx - 1
        return pltpu.make_async_remote_copy(
            src_ref=WPK.at[side], dst_ref=WEB.at[k], send_sem=wssem.at[side],
            recv_sem=wrsem.at[k], device_id=(dest, gy), device_id_type=MESH)

    def sn_copy(side, k):
        dest = 0 if side == 0 else ngy - 1
        return pltpu.make_async_remote_copy(
            src_ref=SPK.at[side], dst_ref=SNB.at[k], send_sem=sssem.at[side],
            recv_sem=srsem.at[k], device_id=(gx, dest), device_id_type=MESH)

    for side in range(2):
        @pl.when(gx != (0 if side == 0 else ngx - 1))
        def _(side=side):
            we_copy(side, gx).start()

        @pl.when(gy != (0 if side == 0 else ngy - 1))
        def _(side=side):
            sn_copy(side, gy).start()

    l_rate.wait()
    l_p.wait()
    l_u.wait()
    l_v.wait()

    def rim_tile(f, z, side):
        at = 0 if side == 0 else rx - 8
        if f == 0:
            return U.at[z, 8 + at:16 + at, :]
        if f == 1:
            return V.at[z, at:at + 8, :]
        return PA.at[z, 8 + at:16 + at, :]

    def keep_rim(side):
        def part(i, _):
            for k in range(10):
                for f in range(3):
                    FO[f, i * 10 + k] = rim_tile(f, i * 10 + k, side)[...]
            return 0

        lax.fori_loop(0, nz // 10, part, 0)

    def blend_x(side):
        me = 0 if side == 0 else ngx - 1
        for k in range(ngx):
            if k == me:
                WEB[k] = WPK[side]
            else:
                we_copy(side, k).wait_recv()
        for i in range(8):
            for k in range(ngx):
                TT[k * sy:(k + 1) * sy, :] = WEB[k, i]
            turned = jnp.transpose(TT[...])
            for half in range(2):
                n = i + 8 * half
                if n >= 3 * BAND:
                    continue
                f, d = n // BAND, n % BAND
                QX[f, :, d if side == 0 else 7 - d, :] = turned[64 * half:64 * half + 64]
        at = 0 if side == 0 else rx - 8
        row = lax.broadcasted_iota(jnp.int32, (8, ly), 0).astype(F32)
        dist = row if side == 0 else 7.0 - row
        lane = lax.broadcasted_iota(jnp.int32, (8, ly), 1).astype(F32)
        rate = RW[at:at + 8].astype(F32)
        weight = jnp.maximum(rate - dist, 0.0) / rate
        south = jnp.where(has_s, 0.0, jnp.maximum(rate - lane, 0.0) / rate)
        north = jnp.where(has_n, 0.0, jnp.maximum(rate - ((ly - 1.0) - lane), 0.0) / rate)
        weight = weight * ((1.0 - south) * (1.0 - north))

        def part(i, _):
            for k in range(10):
                for f in range(3):
                    tile = rim_tile(f, i * 10 + k, side)
                    tile[...] = tile[...] + weight * (QX[f, i * 10 + k] - FO[f, i * 10 + k])
            return 0

        lax.fori_loop(0, nz // 10, part, 0)

    def blend_y(side):
        me = 0 if side == 0 else ngy - 1
        for k in range(ngy):
            if k == me:
                SNB[k] = SPK[side]
            else:
                sn_copy(side, k).wait_recv()
        for k in range(ngy):
            for q in range(4):
                for f in range(3):
                    at = (q * 3 + f) * sx
                    QQ[f, q, k * sx:(k + 1) * sx, :] = SNB[k, at:at + sx, :]
        lane = lax.broadcasted_iota(jnp.int32, (rows, ly), 1).astype(F32)
        dist = lane if side == 0 else (ly - 1.0) - lane

        def part(g, _):
            at = pl.multiple_of(g * rows, 8)
            rate = RW[pl.ds(at, rows)].astype(F32)
            weight = jnp.maximum(rate - dist, 0.0) / rate
            for f in range(3):
                for z in range(nz):
                    shift = ((0 if side == 0 else 120) + 128 - 8 * (z % 16)) % 128
                    slab = pltpu.roll(QQ[f, z // 16, pl.ds(at, rows)], shift, 1)
                    if f == 0:
                        dst = U.at[z, pl.ds(at + 8, rows), :]
                    elif f == 1:
                        dst = V.at[z, pl.ds(at, rows), :]
                    else:
                        dst = PA.at[z, pl.ds(at + 8, rows), :]
                    old = dst[...]
                    dst[...] = old + weight * (slab - old)
            return 0

        lax.fori_loop(0, GROUPS, part, 0)

    QX[...] = jnp.zeros_like(QX)
    for side in range(2):
        @pl.when(gx == (0 if side == 0 else ngx - 1))
        def _(side=side):
            keep_rim(side)
    for side in range(2):
        @pl.when(gy == (0 if side == 0 else ngy - 1))
        def _(side=side):
            blend_y(side)

    pair = lax.broadcasted_iota(jnp.int32, (rows, ly), 1) // 2
    lane_r = lax.broadcasted_iota(jnp.int32, (rows, ly), 1)
    rim = (lane_r == 0) | (lane_r == ly - 1)
    even = lax.rem(lane_r, 2) == 0

    def put(acc, value, z):
        return jnp.where(pair == z, pltpu.roll(value, (2 * z + 1) % 128, 1), acc)

    def own_rows(g):
        return pl.ds(pl.multiple_of(8 + g * rows, 8), rows)

    def all_rows(g):
        return pl.ds(pl.multiple_of(g * rows, 8), rows)

    def in_order(i):
        late = jnp.where(i == GROUPS - 1, 0, jnp.where(i == 0, GROUPS - 1, i))
        both = jnp.where(i == 0, 0, jnp.where(i == 1, GROUPS - 1, i - 1))
        return jnp.where(gx == 0, late, jnp.where(gx == ngx - 1, i, both))

    def put_edges(par, g, acc):
        EB[par, all_rows(g)] = acc
        ES[par, all_rows(g)] = jnp.where(even, pltpu.roll(acc, 127, 1), pltpu.roll(acc, 1, 1))

    def x_west(par):
        return pltpu.make_async_remote_copy(
            src_ref=P[par].at[:, pl.ds(8, 1), :], dst_ref=P[par].at[:, pl.ds(8 + rx, 1), :],
            send_sem=ssem.at[0, par], recv_sem=rsem.at[0, par],
            device_id=(gx - 1, gy), device_id_type=MESH)

    def x_east(par):
        return pltpu.make_async_remote_copy(
            src_ref=P[par].at[:, pl.ds(7 + rx, 1), :], dst_ref=P[par].at[:, pl.ds(7, 1), :],
            send_sem=ssem.at[1, par], recv_sem=rsem.at[1, par],
            device_id=(gx + 1, gy), device_id_type=MESH)

    def u_east():
        return pltpu.make_async_remote_copy(
            src_ref=U.at[:, pl.ds(7 + rx, 1), :], dst_ref=U.at[:, pl.ds(7, 1), :],
            send_sem=ssem.at[10, 0], recv_sem=rsem.at[10, 0],
            device_id=(gx + 1, gy), device_id_type=MESH)

    def y_north(par, g):
        return pltpu.make_async_remote_copy(
            src_ref=ES.at[par, all_rows(g)], dst_ref=RS.at[par, all_rows(g)],
            send_sem=ssem.at[2 + g, par], recv_sem=rsem.at[2 + g, par],
            device_id=(gx, gy + 1), device_id_type=MESH)

    def y_south(par, g):
        return pltpu.make_async_remote_copy(
            src_ref=ES.at[par, all_rows(g)], dst_ref=RN.at[par, all_rows(g)],
            send_sem=ssem.at[6 + g, par], recv_sem=rsem.at[6 + g, par],
            device_id=(gx, gy - 1), device_id_type=MESH)

    def v_north(g):
        return pltpu.make_async_remote_copy(
            src_ref=EV.at[all_rows(g)], dst_ref=RV.at[all_rows(g)],
            send_sem=ssem.at[11 + g, 0], recv_sem=rsem.at[11 + g, 0],
            device_id=(gx, gy + 1), device_id_type=MESH)

    def send_group(par, g):
        @pl.when((g == 0) & has_w)
        def _():
            x_west(par).start()

        @pl.when((g == 0) & jnp.logical_not(has_w))
        def _():
            def part(i, _):
                for k in range(10):
                    P[par][i * 10 + k, 7:8, :] = P[par][i * 10 + k, 8:9, :]
                return 0

            lax.fori_loop(0, nz // 10, part, 0)

        @pl.when((g == GROUPS - 1) & has_e)
        def _():
            x_east(par).start()

        @pl.when(has_n)
        def _():
            y_north(par, g).start()

        @pl.when(has_s)
        def _():
            y_south(par, g).start()

    def wait_group(par, g):
        @pl.when((g == 0) & has_w)
        def _():
            x_east(par).wait_recv()
            x_west(par).wait_send()

        @pl.when((g == GROUPS - 1) & has_e)
        def _():
            x_west(par).wait_recv()
            x_east(par).wait_send()

        @pl.when(g == GROUPS - 1)
        def _():
            def part(i, _):
                for k in range(10):
                    z = i * 10 + k
                    S[z, rx:rx + 1, :] = S[z, rx:rx + 1, :] + P[par][z, 8 + rx:9 + rx, :]
                return 0

            lax.fori_loop(0, nz // 10, part, 0)

        @pl.when(has_n)
        def _():
            y_south(par, g).wait_recv()
            y_north(par, g).wait_send()

        @pl.when(has_s)
        def _():
            y_north(par, g).wait_recv()
            y_south(par, g).wait_send()

    @pl.when(jnp.logical_not(has_w))
    def _():
        U[:, 7, :] = jnp.zeros((nz, ly), F32)

    @pl.when(jnp.logical_not(has_e))
    def _():
        for par in range(2):
            P[par][:, 8 + rx, :] = jnp.zeros((nz, ly), F32)

    @pl.when(jnp.logical_not(has_n))
    def _():
        RN[...] = jnp.zeros_like(RN)

    @pl.when(jnp.logical_not(has_s))
    def _():
        RV[...] = jnp.zeros_like(RV)

    def first(i, _):
        g = in_order(i)
        acc = jnp.zeros((rows, ly), F32)
        for z in range(nz):
            acc = put(acc, PA[z, own_rows(g)], z)
        put_edges(0, g, acc)
        send_group(0, g)
        return 0

    def first_v(i, _):
        g = in_order(i)
        acc = jnp.zeros((rows, ly), F32)
        for z in range(nz):
            acc = put(acc, V[z, all_rows(g)], z)
        EV[all_rows(g)] = acc

        @pl.when(has_n)
        def _():
            v_north(g).start()

        return 0

    SN[...] = jnp.zeros_like(SN)
    S[:, rx, :] = jnp.zeros((nz, ly), F32)
    first_lane = lane_r == 0
    last_lane = lane_r == ly - 1

    def divergence(i, _):
        g = in_order(i)

        @pl.when(has_n)
        def _():
            v_north(g).wait_send()

        @pl.when(has_s)
        def _():
            v_north(g).wait_recv()

        halo_v = RV[all_rows(g)]
        for z in range(nz):
            u = U[z, own_rows(g)]
            uw = U[z, pl.ds(7 + g * rows, rows)]
            v = V[z, all_rows(g)]
            vs = jnp.where(first_lane, pltpu.roll(halo_v, (128 - 2 * z) % 128, 1),
                           pltpu.roll(v, 1, 1))
            E[z, all_rows(g)] = 0.3 * ((u - uw) + (v - vs))
            S[z, all_rows(g)] = jnp.zeros((rows, ly), F32)
        return 0

    @pl.when(has_e)
    def _():
        u_east().start()

    lax.fori_loop(0, GROUPS - 1, first, 0)
    lax.fori_loop(0, GROUPS - 1, first_v, 0)

    @pl.when(has_e)
    def _():
        u_east().wait_send()

    @pl.when(has_w)
    def _():
        u_east().wait_recv()

    lax.fori_loop(0, GROUPS - 1, divergence, 0)
    for side in range(2):
        @pl.when(gx == (0 if side == 0 else ngx - 1))
        def _(side=side):
            blend_x(side)
    for part_of in (first, first_v, divergence):
        lax.fori_loop(GROUPS - 1, GROUPS, part_of, 0)

    l_w.wait()

    def corrections(cur, g):
        rn = RN[cur, all_rows(g)]
        rs = jnp.where(has_s, RS[cur, all_rows(g)], EB[cur, all_rows(g)])
        SN[all_rows(g)] = SN[all_rows(g)] + rn
        return jnp.where(even, rn, rs) - ES[cur, all_rows(g)]

    def forward(cur, nxt, g):
        rinv = 1.0 / R[all_rows(g)]
        k_g = corrections(cur, g)

        def get_q(z):
            p = P[cur][z, own_rows(g)]
            pe = P[cur][z, pl.ds(9 + g * rows, rows)]
            pw = P[cur][z, pl.ds(7 + g * rows, rows)]
            ns = pltpu.roll(p, 1, 1) + pltpu.roll(p, 127, 1)
            k = jnp.where(rim, pltpu.roll(k_g, (255 - 2 * z) % 128, 1), 0.0)
            total = (pe + pw) + (ns + k)
            e = E[z, all_rows(g)] + 0.09 * (4.0 * p - total)
            E[z, all_rows(g)] = e
            S[z, all_rows(g)] = S[z, all_rows(g)] + p
            q = p - e
            P[nxt][z, own_rows(g)] = q
            return q

        q, d = get_q(0), jnp.zeros((rows, ly), F32)
        for z in range(nz):
            qn = get_q(z + 1) if z < nz - 1 else None
            diff = q - qn if z < nz - 1 else q
            rhs = W[z, all_rows(g)] + 0.5 * diff
            d = G[z, all_rows(g)] * (rinv * rhs + d)
            W[z, all_rows(g)] = d
            q = qn

    def backward(nxt, g, edges):
        acc = jnp.zeros((rows, ly), F32)
        w = W[nz - 1, all_rows(g)]
        h = 0.5 * w
        for z in range(nz - 2, -2, -1):
            p = P[nxt][z + 1, own_rows(g)] - h
            if z >= 0:
                w = W[z, all_rows(g)] + G[z, all_rows(g)] * w
                W[z, all_rows(g)] = w
                h = 0.5 * w
                p = p + h
            P[nxt][z + 1, own_rows(g)] = p
            if edges:
                acc = put(acc, p, z + 1)
        if edges:
            put_edges(nxt, g, acc)

    def step(cur, nxt):
        def part(i, _):
            g = in_order(i)
            wait_group(cur, g)
            forward(cur, nxt, g)
            backward(nxt, g, True)
            send_group(nxt, g)
            return 0

        lax.fori_loop(0, GROUPS, part, 0)

    def two_steps(i, _):
        step(0, 1)
        step(1, 0)
        return 0

    lax.fori_loop(0, (STEPS - 2) // 2, two_steps, 0)
    step(0, 1)

    def last(i, _):
        g = in_order(i)
        wait_group(1, g)
        forward(1, 0, g)
        backward(0, g, False)
        return 0

    lax.fori_loop(0, GROUPS, last, 0)

    for side in range(2):
        @pl.when(gx != (0 if side == 0 else ngx - 1))
        def _(side=side):
            we_copy(side, gx).wait_send()

        @pl.when(gy != (0 if side == 0 else ngy - 1))
        def _(side=side):
            sn_copy(side, gy).wait_send()


def finish(nz, rx, ly, W, PA, U, V, S, SN, uo_hbm, vo_hbm, wo_hbm, po_hbm, UO, VO, osem):
    rows = rx // GROUPS
    store_w = pltpu.make_async_copy(W, wo_hbm, osem.at[0, GROUPS])
    store_p = pltpu.make_async_copy(PA.at[:, pl.ds(8, rx), :], po_hbm, osem.at[1, GROUPS])
    store_w.start()
    store_p.start()
    last_lane = lax.broadcasted_iota(jnp.int32, (rows, ly), 1) == ly - 1

    def store(k, g):
        src, dst = ((UO, uo_hbm), (VO, vo_hbm))[k]
        at = pl.ds(pl.multiple_of(g * rows, 8), rows)
        return pltpu.make_async_copy(src.at[:, at, :], dst.at[:, at, :], osem.at[k, g])

    def winds(g, _):
        at = pl.ds(pl.multiple_of(g * rows, 8), rows)
        halo = SN[at]
        for z in range(nz):
            t = S[z, at]
            te = S[z, pl.ds(g * rows + 1, rows)]
            tn = jnp.where(last_lane, pltpu.roll(halo, (255 - 2 * z) % 128, 1),
                           pltpu.roll(t, 127, 1))
            UO[z, at] = U[z, pl.ds(pl.multiple_of(g * rows + 8, 8), rows)] - 0.3 * (te - t)
            VO[z, at] = V[z, at] - 0.3 * (tn - t)
        store(0, g).start()
        store(1, g).start()
        return 0

    lax.fori_loop(0, GROUPS, winds, 0)
    store_w.wait()
    store_p.wait()
    for g in range(GROUPS):
        store(0, g).wait()
        store(1, g).wait()


def per_device(ngx, ngy, u, v, w, p, r, we, sn, rate):
    nz, rx, ly = p.shape
    we = jnp.transpose(we, (0, 1, 3, 4, 2))
    sn = jnp.transpose(sn, (0, 1, 3, 4, 2))
    field = jax.ShapeDtypeStruct((nz, rx, ly), F32)
    vm = lambda *s: pltpu.VMEM(s, F32)
    hbm = pl.BlockSpec(memory_space=pltpu.HBM)
    vmem = pl.BlockSpec(memory_space=pltpu.VMEM)
    dma = pltpu.SemaphoreType.DMA
    sx = rx // ngy
    scratch = [
        vm(nz, rx + 16, ly), vm(nz, rx, ly), vm(nz, rx, ly),
        vm(rx, ly), pltpu.VMEM((rx, ly), jnp.int32),
        vm(2, 3, BAND, ly // ngx, nz), vm(2, 3, BAND, sx, nz),
        vm(2, 8, ly // ngx, 128), vm(2, 12 * sx, 128),
        vm(ngx, 8, ly // ngx, 128), vm(ngy, 12 * sx, 128),
        vm(128, 128), vm(64, 8, 128), vm(64, 8, 128), vm(3, 4, rx, 128), vm(3, nz, 8, ly),
        vm(3, 64, 8, ly),
        vm(2, rx, ly), vm(2, rx, ly), vm(2, rx, ly), vm(2, rx, ly), vm(rx, ly), vm(rx, ly),
        dma((8,)), dma((11 + GROUPS, 2)), dma((11 + GROUPS, 2)),
        dma((2,)), dma((ngx,)), dma((2,)), dma((ngy,)),
    ]
    state = pl.pallas_call(
        functools.partial(kernel, ngx, ngy, nz, rx, ly),
        out_shape=(vm(nz, rx, ly), vm(nz, rx + 16, ly), vm(nz, rx + 8, ly), vm(nz, rx, ly),
                   vm(nz, rx + 8, ly), vm(rx, ly)),
        in_specs=[hbm] * 8,
        out_specs=(vmem,) * 6,
        scratch_shapes=scratch,
        compiler_params=pltpu.CompilerParams(collective_id=0, has_side_effects=True,
                                             vmem_limit_bytes=30 * 1024 * 1024),
    )(*(pltpu.with_memory_space_constraint(x, pltpu.HBM) for x in (u, v, w, p, r, we, sn, rate)))
    return pl.pallas_call(
        functools.partial(finish, nz, rx, ly),
        out_shape=(field,) * 4,
        in_specs=[vmem] * 6,
        out_specs=(hbm,) * 4,
        scratch_shapes=[vm(nz, rx, ly), vm(nz, rx, ly), dma((2, GROUPS + 1))],
        compiler_params=pltpu.CompilerParams(vmem_limit_bytes=16 * 1024 * 1024),
    )(*state)


def solution(mesh):
    ngx, ngy = mesh.shape["gx"], mesh.shape["gy"]
    grid = PS(None, "gx", "gy")
    return jax.shard_map(
        functools.partial(per_device, ngx, ngy),
        mesh=mesh,
        in_specs=(grid,) * 4 + (
            PS("gx", "gy"),
            PS(None, None, None, None, ("gy", "gx")),
            PS(None, None, None, None, ("gx", "gy")),
            PS("gx", "gy"),
        ),
        out_specs=(grid,) * 4,
        check_vma=False,
    )
```

```python
import functools

import jax
import jax.numpy as jnp
from jax import lax
from jax.experimental import pallas as pl
from jax.experimental.pallas import tpu as pltpu
from jax.sharding import PartitionSpec as PS

MESH = pl.DeviceIdType.MESH
STEPS = 6
GROUPS = 4
BAND = 5
F32 = jnp.float32


def kernel(ngx, ngy, nz, rx, ly,
           u_hbm, v_hbm, w_hbm, p_hbm, r_hbm, we_hbm, sn_hbm, rate_hbm,
           W, PA, U, V, S, SN,
           PB, E, G, R, RW, WEL, SNL, WPK, SPK, WEB, SNB, TT, BB, BN, QQ, FO,
           QX, EB, ES, RN, RS, EV, RV,
           lsem, ssem, rsem, wssem, wrsem, sssem, srsem):
    P = (PA, PB)
    gx = lax.axis_index("gx")
    gy = lax.axis_index("gy")
    has_w, has_e = gx > 0, gx < ngx - 1
    has_s, has_n = gy > 0, gy < ngy - 1
    rows = rx // GROUPS
    sy = ly // ngx
    sx = rx // ngy

    def load(i, src, dst):
        c = pltpu.make_async_copy(src, dst, lsem.at[i])
        c.start()
        return c

    l_we = load(5, we_hbm, WEL)
    l_sn = load(6, sn_hbm, SNL)
    l_r = load(4, r_hbm, R)
    l_rate = load(7, rate_hbm, RW)
    l_p = load(3, p_hbm, PA.at[:, pl.ds(8, rx), :])
    l_u = load(0, u_hbm, U.at[:, pl.ds(8, rx), :])
    l_v = load(1, v_hbm, V)
    l_w = load(2, w_hbm, W)

    barrier = pltpu.get_barrier_semaphore()

    def peers(me, other, n):
        return (other != me) & (
            (other == me - 1) | (other == me + 1) | (other == 0) | (other == n - 1)
            | (me == 0) | (me == n - 1))

    count = jnp.int32(0)
    for k in range(ngx):
        ok = peers(gx, k, ngx)
        count = count + jnp.where(ok, 1, 0)

        @pl.when(ok)
        def _(k=k):
            pl.semaphore_signal(barrier, inc=1, device_id=(k, gy), device_id_type=MESH)
    for k in range(ngy):
        ok = peers(gy, k, ngy)
        count = count + jnp.where(ok, 1, 0)

        @pl.when(ok)
        def _(k=k):
            pl.semaphore_signal(barrier, inc=1, device_id=(gx, k), device_id_type=MESH)

    WPK[...] = jnp.zeros_like(WPK)
    BB[...] = jnp.zeros_like(BB)
    BN[...] = jnp.zeros_like(BN)
    TT[...] = jnp.zeros_like(TT)
    l_we.wait()
    l_sn.wait()
    for side in range(2):
        for i in range(3 * BAND):
            f, d = i // BAND, i % BAND
            lo = 0 if i < 8 else 64
            WPK[side, i % 8, :, lo:lo + nz] = WEL[side, f, d]

    wide = 6 * sx
    per = 128 // wide
    for lot in range(0, BAND, per):
        for d in range(lot, min(lot + per, BAND)):
            for side in range(2):
                for f in range(3):
                    at = (d - lot) * wide + (side * 3 + f) * sx
                    TT[at:at + sx, 0:nz] = SNL[side, f, d]
        turned = jnp.transpose(TT[...])[:64]
        for d in range(lot, min(lot + per, BAND)):
            shift = (128 - (d - lot) * wide) % 128
            moved = pltpu.roll(turned, shift, 1) if shift else turned
            BB[:, d, :] = moved
            BN[:, 7 - d, :] = moved
    for q in range(4):
        for side, ref in enumerate((BB, BN)):
            block = jnp.transpose(ref[16 * q:16 * q + 16].reshape(128, 128))
            for f in range(3):
                at = (f * 4 + q) * sx
                SPK[side, at:at + sx, :] = block[(side * 3 + f) * sx:(side * 3 + f + 1) * sx]

    l_r.wait()
    r_all = R[...]
    base = 1.0 + 2.0 * r_all

    def factor(z, prev):
        g = r_all / (base - r_all * prev)
        G[z] = g
        return g

    lax.fori_loop(0, nz, factor, jnp.zeros_like(r_all))

    pl.semaphore_wait(barrier, count)

    def we_copy(side, k):
        dest = 0 if side == 0 else ngx - 1
        return pltpu.make_async_remote_copy(
            src_ref=WPK.at[side], dst_ref=WEB.at[k], send_sem=wssem.at[side],
            recv_sem=wrsem.at[k], device_id=(dest, gy), device_id_type=MESH)

    def sn_rows(part):
        return pl.ds(0, 8 * sx) if part else pl.ds(8 * sx, 4 * sx)

    def sn_copy(side, k, part):
        dest = 0 if side == 0 else ngy - 1
        return pltpu.make_async_remote_copy(
            src_ref=SPK.at[side, sn_rows(part)], dst_ref=SNB.at[k, sn_rows(part)],
            send_sem=sssem.at[side, part], recv_sem=srsem.at[k, part],
            device_id=(gx, dest), device_id_type=MESH)

    for act in ("start", "wait_send"):
        for part in range(2):
            for side in range(2):
                @pl.when(gy != (0 if side == 0 else ngy - 1))
                def _(side=side):
                    getattr(sn_copy(side, gy, part), act)()
    for side in range(2):
        @pl.when(gx != (0 if side == 0 else ngx - 1))
        def _(side=side):
            we_copy(side, gx).start()

    l_rate.wait()
    l_p.wait()
    l_u.wait()
    l_v.wait()

    def rim_tile(f, z, side):
        at = 0 if side == 0 else rx - 8
        if f == 0:
            return U.at[z, 8 + at:16 + at, :]
        if f == 1:
            return V.at[z, at:at + 8, :]
        return PA.at[z, 8 + at:16 + at, :]

    def keep_rim(side):
        def part(i, _):
            for k in range(10):
                for f in range(3):
                    FO[f, i * 10 + k] = rim_tile(f, i * 10 + k, side)[...]
            return 0

        lax.fori_loop(0, nz // 10, part, 0)

    def blend_x(side):
        me = 0 if side == 0 else ngx - 1
        for k in range(ngx):
            if k == me:
                WEB[k] = WPK[side]
            else:
                we_copy(side, k).wait_recv()
        for i in range(8):
            for k in range(ngx):
                TT[k * sy:(k + 1) * sy, :] = WEB[k, i]
            turned = jnp.transpose(TT[...])
            for half in range(2):
                n = i + 8 * half
                if n >= 3 * BAND:
                    continue
                f, d = n // BAND, n % BAND
                QX[f, :, d if side == 0 else 7 - d, :] = turned[64 * half:64 * half + 64]
        at = 0 if side == 0 else rx - 8
        row = lax.broadcasted_iota(jnp.int32, (8, ly), 0).astype(F32)
        dist = row if side == 0 else 7.0 - row
        lane = lax.broadcasted_iota(jnp.int32, (8, ly), 1).astype(F32)
        rate = RW[at:at + 8].astype(F32)
        weight = jnp.maximum(rate - dist, 0.0) / rate
        south = jnp.where(has_s, 0.0, jnp.maximum(rate - lane, 0.0) / rate)
        north = jnp.where(has_n, 0.0, jnp.maximum(rate - ((ly - 1.0) - lane), 0.0) / rate)
        weight = weight * ((1.0 - south) * (1.0 - north))

        def part(i, _):
            for k in range(10):
                for f in range(3):
                    tile = rim_tile(f, i * 10 + k, side)
                    tile[...] = tile[...] + weight * (QX[f, i * 10 + k] - FO[f, i * 10 + k])
            return 0

        lax.fori_loop(0, nz // 10, part, 0)

    def gather_y(side, part):
        me = 0 if side == 0 else ngy - 1
        for k in range(ngy):
            if k == me:
                SNB[k, sn_rows(part)] = SPK[side, sn_rows(part)]
            else:
                sn_copy(side, k, part).wait_recv()
        for k in range(ngy):
            for f in ((0, 1) if part else (2,)):
                for q in range(4):
                    at = (f * 4 + q) * sx
                    QQ[f, q, k * sx:(k + 1) * sx, :] = SNB[k, at:at + sx, :]

    def blend_fields(side, fields):
        lane = lax.broadcasted_iota(jnp.int32, (rows, ly), 1).astype(F32)
        dist = lane if side == 0 else (ly - 1.0) - lane

        def part(g, _):
            at = pl.multiple_of(g * rows, 8)
            rate = RW[pl.ds(at, rows)].astype(F32)
            weight = jnp.maximum(rate - dist, 0.0) / rate
            for f in fields:
                for z in range(nz):
                    shift = ((0 if side == 0 else 120) + 128 - 8 * (z % 16)) % 128
                    slab = pltpu.roll(QQ[f, z // 16, pl.ds(at, rows)], shift, 1)
                    if f == 0:
                        dst = U.at[z, pl.ds(at + 8, rows), :]
                    elif f == 1:
                        dst = V.at[z, pl.ds(at, rows), :]
                    else:
                        dst = PA.at[z, pl.ds(at + 8, rows), :]
                    old = dst[...]
                    dst[...] = old + weight * (slab - old)
            return 0

        lax.fori_loop(0, GROUPS, part, 0)

    QX[...] = jnp.zeros_like(QX)
    for side in range(2):
        @pl.when(gx == (0 if side == 0 else ngx - 1))
        def _(side=side):
            keep_rim(side)
    for side in range(2):
        @pl.when(gy == (0 if side == 0 else ngy - 1))
        def _(side=side):
            gather_y(side, 0)
            blend_fields(side, (2,))

    pair = lax.broadcasted_iota(jnp.int32, (rows, ly), 1) // 2
    lane_r = lax.broadcasted_iota(jnp.int32, (rows, ly), 1)
    rim = (lane_r == 0) | (lane_r == ly - 1)
    even = lax.rem(lane_r, 2) == 0

    def put(acc, value, z):
        return jnp.where(pair == z, pltpu.roll(value, (2 * z + 1) % 128, 1), acc)

    def own_rows(g):
        return pl.ds(pl.multiple_of(8 + g * rows, 8), rows)

    def all_rows(g):
        return pl.ds(pl.multiple_of(g * rows, 8), rows)

    def in_order(i):
        late = jnp.where(i == GROUPS - 1, 0, jnp.where(i == 0, GROUPS - 1, i))
        both = jnp.where(i == 0, 0, jnp.where(i == 1, GROUPS - 1, i - 1))
        return jnp.where(gx == 0, late, jnp.where(gx == ngx - 1, i, both))

    def put_edges(par, g, acc):
        EB[par, all_rows(g)] = acc
        ES[par, all_rows(g)] = jnp.where(even, pltpu.roll(acc, 127, 1), pltpu.roll(acc, 1, 1))

    def x_west(par):
        return pltpu.make_async_remote_copy(
            src_ref=P[par].at[:, pl.ds(8, 1), :], dst_ref=P[par].at[:, pl.ds(8 + rx, 1), :],
            send_sem=ssem.at[0, par], recv_sem=rsem.at[0, par],
            device_id=(gx - 1, gy), device_id_type=MESH)

    def x_east(par):
        return pltpu.make_async_remote_copy(
            src_ref=P[par].at[:, pl.ds(7 + rx, 1), :], dst_ref=P[par].at[:, pl.ds(7, 1), :],
            send_sem=ssem.at[1, par], recv_sem=rsem.at[1, par],
            device_id=(gx + 1, gy), device_id_type=MESH)

    def u_east():
        return pltpu.make_async_remote_copy(
            src_ref=U.at[:, pl.ds(7 + rx, 1), :], dst_ref=U.at[:, pl.ds(7, 1), :],
            send_sem=ssem.at[10, 0], recv_sem=rsem.at[10, 0],
            device_id=(gx + 1, gy), device_id_type=MESH)

    def y_north(par, g):
        return pltpu.make_async_remote_copy(
            src_ref=ES.at[par, all_rows(g)], dst_ref=RS.at[par, all_rows(g)],
            send_sem=ssem.at[2 + g, par], recv_sem=rsem.at[2 + g, par],
            device_id=(gx, gy + 1), device_id_type=MESH)

    def y_south(par, g):
        return pltpu.make_async_remote_copy(
            src_ref=ES.at[par, all_rows(g)], dst_ref=RN.at[par, all_rows(g)],
            send_sem=ssem.at[6 + g, par], recv_sem=rsem.at[6 + g, par],
            device_id=(gx, gy - 1), device_id_type=MESH)

    def v_north(g):
        return pltpu.make_async_remote_copy(
            src_ref=EV.at[all_rows(g)], dst_ref=RV.at[all_rows(g)],
            send_sem=ssem.at[11 + g, 0], recv_sem=rsem.at[11 + g, 0],
            device_id=(gx, gy + 1), device_id_type=MESH)

    def send_x(par, g):
        @pl.when((g == 0) & has_w)
        def _():
            x_west(par).start()

        @pl.when((g == GROUPS - 1) & has_e)
        def _():
            x_east(par).start()

    def send_y(par, g):
        @pl.when(has_n)
        def _():
            y_north(par, g).start()

        @pl.when(has_s)
        def _():
            y_south(par, g).start()

        @pl.when((g == 0) & jnp.logical_not(has_w))
        def _():
            def part(i, _):
                for k in range(10):
                    P[par][i * 10 + k, 7:8, :] = P[par][i * 10 + k, 8:9, :]
                return 0

            lax.fori_loop(0, nz // 10, part, 0)

    def wait_group(par, g):
        @pl.when((g == 0) & has_w)
        def _():
            x_east(par).wait_recv()
            x_west(par).wait_send()

        @pl.when((g == GROUPS - 1) & has_e)
        def _():
            x_west(par).wait_recv()
            x_east(par).wait_send()

        @pl.when(has_n)
        def _():
            y_south(par, g).wait_recv()
            y_north(par, g).wait_send()

        @pl.when(has_s)
        def _():
            y_north(par, g).wait_recv()
            y_south(par, g).wait_send()

    def s_west():
        return pltpu.make_async_remote_copy(
            src_ref=S.at[:, pl.ds(0, 1), :], dst_ref=S.at[:, pl.ds(rx, 1), :],
            send_sem=ssem.at[10, 1], recv_sem=rsem.at[10, 1],
            device_id=(gx - 1, gy), device_id_type=MESH)

    @pl.when(jnp.logical_not(has_w))
    def _():
        U[:, 7, :] = jnp.zeros((nz, ly), F32)

    @pl.when(jnp.logical_not(has_e))
    def _():
        for par in range(2):
            P[par][:, 8 + rx, :] = jnp.zeros((nz, ly), F32)

    @pl.when(jnp.logical_not(has_n))
    def _():
        RN[...] = jnp.zeros_like(RN)

    @pl.when(jnp.logical_not(has_s))
    def _():
        RV[...] = jnp.zeros_like(RV)

    def first(i, _):
        g = in_order(i)
        acc = jnp.zeros((rows, ly), F32)
        for z in range(nz):
            acc = put(acc, PA[z, own_rows(g)], z)
        send_x(0, g)
        put_edges(0, g, acc)
        send_y(0, g)
        return 0

    def first_v(i, _):
        g = in_order(i)
        acc = jnp.zeros((rows, ly), F32)
        for z in range(nz):
            acc = put(acc, V[z, all_rows(g)], z)
        EV[all_rows(g)] = acc

        @pl.when(has_n)
        def _():
            v_north(g).start()

        return 0

    SN[...] = jnp.zeros_like(SN)

    @pl.when(jnp.logical_not(has_e))
    def _():
        S[:, rx, :] = jnp.zeros((nz, ly), F32)

    first_lane = lane_r == 0
    last_lane = lane_r == ly - 1

    def divergence(i, _):
        g = in_order(i)

        @pl.when(has_n)
        def _():
            v_north(g).wait_send()

        @pl.when(has_s)
        def _():
            v_north(g).wait_recv()

        halo_v = RV[all_rows(g)]
        for z in range(nz):
            u = U[z, own_rows(g)]
            uw = U[z, pl.ds(7 + g * rows, rows)]
            v = V[z, all_rows(g)]
            vs = jnp.where(first_lane, pltpu.roll(halo_v, (128 - 2 * z) % 128, 1),
                           pltpu.roll(v, 1, 1))
            E[z, all_rows(g)] = 0.3 * ((u - uw) + (v - vs))
            S[z, all_rows(g)] = jnp.zeros((rows, ly), F32)
        return 0

    lax.fori_loop(0, GROUPS - 1, first, 0)
    for side in range(2):
        @pl.when(gy == (0 if side == 0 else ngy - 1))
        def _(side=side):
            gather_y(side, 1)
            blend_fields(side, (0, 1))

    @pl.when(has_e)
    def _():
        u_east().start()

    lax.fori_loop(0, GROUPS - 1, first_v, 0)

    @pl.when(has_e)
    def _():
        u_east().wait_send()

    @pl.when(has_w)
    def _():
        u_east().wait_recv()

    lax.fori_loop(0, GROUPS - 1, divergence, 0)
    for side in range(2):
        @pl.when(gx == (0 if side == 0 else ngx - 1))
        def _(side=side):
            blend_x(side)
    for part_of in (first, first_v, divergence):
        lax.fori_loop(GROUPS - 1, GROUPS, part_of, 0)

    l_w.wait()

    def corrections(cur, g):
        rn = RN[cur, all_rows(g)]
        rs = jnp.where(has_s, RS[cur, all_rows(g)], EB[cur, all_rows(g)])
        SN[all_rows(g)] = SN[all_rows(g)] + rn
        return jnp.where(even, rn, rs) - ES[cur, all_rows(g)]

    def forward(cur, nxt, g):
        rinv = 1.0 / R[all_rows(g)]
        k_g = corrections(cur, g)

        def get_q(z):
            p = P[cur][z, own_rows(g)]
            pe = P[cur][z, pl.ds(9 + g * rows, rows)]
            pw = P[cur][z, pl.ds(7 + g * rows, rows)]
            ns = pltpu.roll(p, 1, 1) + pltpu.roll(p, 127, 1)
            k = jnp.where(rim, pltpu.roll(k_g, (255 - 2 * z) % 128, 1), 0.0)
            total = (pe + pw) + (ns + k)
            e = E[z, all_rows(g)] + 0.09 * (4.0 * p - total)
            E[z, all_rows(g)] = e
            S[z, all_rows(g)] = S[z, all_rows(g)] + p
            q = p - e
            P[nxt][z, own_rows(g)] = q
            return q

        q, d = get_q(0), jnp.zeros((rows, ly), F32)
        for z in range(nz):
            qn = get_q(z + 1) if z < nz - 1 else None
            diff = q - qn if z < nz - 1 else q
            rhs = W[z, all_rows(g)] + 0.5 * diff
            d = G[z, all_rows(g)] * (rinv * rhs + d)
            W[z, all_rows(g)] = d
            q = qn

    def backward(nxt, g, edges):
        acc = jnp.zeros((rows, ly), F32)
        w = W[nz - 1, all_rows(g)]
        h = 0.5 * w
        for z in range(nz - 2, -2, -1):
            p = P[nxt][z + 1, own_rows(g)] - h
            if z >= 0:
                w = W[z, all_rows(g)] + G[z, all_rows(g)] * w
                W[z, all_rows(g)] = w
                h = 0.5 * w
                p = p + h
            P[nxt][z + 1, own_rows(g)] = p
            if edges:
                acc = put(acc, p, z + 1)
        if edges:
            send_x(nxt, g)
            put_edges(nxt, g, acc)

    def step(cur, nxt, share=False):
        def part(i, _):
            g = in_order(i)
            wait_group(cur, g)
            forward(cur, nxt, g)
            backward(nxt, g, True)
            send_y(nxt, g)
            if share:
                @pl.when((g == 0) & has_w)
                def _():
                    s_west().start()
            return 0

        lax.fori_loop(0, GROUPS, part, 0)

    def two_steps(i, _):
        step(0, 1)
        step(1, 0)
        return 0

    lax.fori_loop(0, (STEPS - 2) // 2, two_steps, 0)
    step(0, 1, share=True)

    def last(i, _):
        g = in_order(i)
        wait_group(1, g)

        @pl.when((g == 0) & has_w)
        def _():
            s_west().wait_send()

        forward(1, 0, g)
        backward(0, g, False)
        return 0

    lax.fori_loop(0, GROUPS, last, 0)

    @pl.when(has_e)
    def _():
        s_west().wait_recv()

        def part(i, _):
            for k in range(10):
                z = i * 10 + k
                S[z, rx:rx + 1, :] = S[z, rx:rx + 1, :] + PB[z, 8 + rx:9 + rx, :]
            return 0

        lax.fori_loop(0, nz // 10, part, 0)

    for side in range(2):
        @pl.when(gx != (0 if side == 0 else ngx - 1))
        def _(side=side):
            we_copy(side, gx).wait_send()


def finish(nz, rx, ly, W, PA, U, V, S, SN, uo_hbm, vo_hbm, wo_hbm, po_hbm, UO, VO, osem):
    rows = rx // GROUPS
    store_w = pltpu.make_async_copy(W, wo_hbm, osem.at[0, GROUPS])
    store_p = pltpu.make_async_copy(PA.at[:, pl.ds(8, rx), :], po_hbm, osem.at[1, GROUPS])
    store_w.start()
    store_p.start()
    last_lane = lax.broadcasted_iota(jnp.int32, (rows, ly), 1) == ly - 1

    def store(k, g):
        src, dst = ((UO, uo_hbm), (VO, vo_hbm))[k]
        at = pl.ds(pl.multiple_of(g * rows, 8), rows)
        return pltpu.make_async_copy(src.at[:, at, :], dst.at[:, at, :], osem.at[k, g])

    def winds(g, _):
        at = pl.ds(pl.multiple_of(g * rows, 8), rows)
        halo = SN[at]
        for z in range(nz):
            t = S[z, at]
            te = S[z, pl.ds(g * rows + 1, rows)]
            tn = jnp.where(last_lane, pltpu.roll(halo, (255 - 2 * z) % 128, 1),
                           pltpu.roll(t, 127, 1))
            UO[z, at] = U[z, pl.ds(pl.multiple_of(g * rows + 8, 8), rows)] - 0.3 * (te - t)
            VO[z, at] = V[z, at] - 0.3 * (tn - t)
        store(0, g).start()
        store(1, g).start()
        return 0

    lax.fori_loop(0, GROUPS, winds, 0)
    store_w.wait()
    store_p.wait()
    for g in range(GROUPS):
        store(0, g).wait()
        store(1, g).wait()


def per_device(ngx, ngy, u, v, w, p, r, we, sn, rate):
    nz, rx, ly = p.shape
    we = jnp.transpose(we, (0, 1, 3, 4, 2))
    sn = jnp.transpose(sn, (0, 1, 3, 4, 2))
    field = jax.ShapeDtypeStruct((nz, rx, ly), F32)
    vm = lambda *s: pltpu.VMEM(s, F32)
    hbm = pl.BlockSpec(memory_space=pltpu.HBM)
    vmem = pl.BlockSpec(memory_space=pltpu.VMEM)
    dma = pltpu.SemaphoreType.DMA
    sx = rx // ngy
    scratch = [
        vm(nz, rx + 16, ly), vm(nz, rx, ly), vm(nz, rx, ly),
        vm(rx, ly), pltpu.VMEM((rx, ly), jnp.int32),
        vm(2, 3, BAND, ly // ngx, nz), vm(2, 3, BAND, sx, nz),
        vm(2, 8, ly // ngx, 128), vm(2, 12 * sx, 128),
        vm(ngx, 8, ly // ngx, 128), vm(ngy, 12 * sx, 128),
        vm(128, 128), vm(64, 8, 128), vm(64, 8, 128), vm(3, 4, rx, 128), vm(3, nz, 8, ly),
        vm(3, 64, 8, ly),
        vm(2, rx, ly), vm(2, rx, ly), vm(2, rx, ly), vm(2, rx, ly), vm(rx, ly), vm(rx, ly),
        dma((8,)), dma((11 + GROUPS, 2)), dma((11 + GROUPS, 2)),
        dma((2,)), dma((ngx,)), dma((2, 2)), dma((ngy, 2)),
    ]
    state = pl.pallas_call(
        functools.partial(kernel, ngx, ngy, nz, rx, ly),
        out_shape=(vm(nz, rx, ly), vm(nz, rx + 16, ly), vm(nz, rx + 8, ly), vm(nz, rx, ly),
                   vm(nz, rx + 8, ly), vm(rx, ly)),
        in_specs=[hbm] * 8,
        out_specs=(vmem,) * 6,
        scratch_shapes=scratch,
        compiler_params=pltpu.CompilerParams(collective_id=0, has_side_effects=True,
                                             vmem_limit_bytes=30 * 1024 * 1024),
    )(*(pltpu.with_memory_space_constraint(x, pltpu.HBM) for x in (u, v, w, p, r, we, sn, rate)))
    return pl.pallas_call(
        functools.partial(finish, nz, rx, ly),
        out_shape=(field,) * 4,
        in_specs=[vmem] * 6,
        out_specs=(hbm,) * 4,
        scratch_shapes=[vm(nz, rx, ly), vm(nz, rx, ly), dma((2, GROUPS + 1))],
        compiler_params=pltpu.CompilerParams(vmem_limit_bytes=16 * 1024 * 1024),
    )(*state)


def solution(mesh):
    ngx, ngy = mesh.shape["gx"], mesh.shape["gy"]
    grid = PS(None, "gx", "gy")
    return jax.shard_map(
        functools.partial(per_device, ngx, ngy),
        mesh=mesh,
        in_specs=(grid,) * 4 + (
            PS("gx", "gy"),
            PS(None, None, None, None, ("gy", "gx")),
            PS(None, None, None, None, ("gx", "gy")),
            PS("gx", "gy"),
        ),
        out_specs=(grid,) * 4,
        check_vma=False,
    )
```

```python
import functools

import jax
import jax.numpy as jnp
from jax import lax
from jax.experimental import pallas as pl
from jax.experimental.pallas import tpu as pltpu
from jax.sharding import PartitionSpec as PS

MESH = pl.DeviceIdType.MESH
STEPS = 6
GROUPS = 4
BAND = 5
F32 = jnp.float32


def kernel(ngx, ngy, nz, rx, ly,
           u_hbm, v_hbm, w_hbm, p_hbm, r_hbm, we_hbm, sn_hbm, rate_hbm,
           W, PA, U, V, S, SN,
           PB, E, G, R, RW, WEL, SNL, WPK, SPK, WEB, SNB, TT, BB, BN, QQ, FO,
           QX, EB, ES, RN, RS, EV, RV,
           lsem, ssem, rsem, wssem, wrsem, sssem, srsem):
    P = (PA, PB)
    gx = lax.axis_index("gx")
    gy = lax.axis_index("gy")
    has_w, has_e = gx > 0, gx < ngx - 1
    has_s, has_n = gy > 0, gy < ngy - 1
    rows = rx // GROUPS
    sy = ly // ngx
    sx = rx // ngy

    def load(i, src, dst):
        c = pltpu.make_async_copy(src, dst, lsem.at[i])
        c.start()
        return c

    l_we = load(5, we_hbm, WEL)
    l_sn = load(6, sn_hbm, SNL)
    l_r = load(4, r_hbm, R)
    l_rate = load(7, rate_hbm, RW)
    l_p = load(3, p_hbm, PA.at[:, pl.ds(8, rx), :])
    l_u = load(0, u_hbm, U.at[:, pl.ds(8, rx), :])
    l_v = load(1, v_hbm, V)
    l_w = load(2, w_hbm, W)

    barrier = pltpu.get_barrier_semaphore()

    def peers(me, other, n):
        return (other != me) & (
            (other == me - 1) | (other == me + 1) | (other == 0) | (other == n - 1)
            | (me == 0) | (me == n - 1))

    count = jnp.int32(0)
    for k in range(ngx):
        ok = peers(gx, k, ngx)
        count = count + jnp.where(ok, 1, 0)

        @pl.when(ok)
        def _(k=k):
            pl.semaphore_signal(barrier, inc=1, device_id=(k, gy), device_id_type=MESH)
    for k in range(ngy):
        ok = peers(gy, k, ngy)
        count = count + jnp.where(ok, 1, 0)

        @pl.when(ok)
        def _(k=k):
            pl.semaphore_signal(barrier, inc=1, device_id=(gx, k), device_id_type=MESH)

    WPK[...] = jnp.zeros_like(WPK)
    BB[...] = jnp.zeros_like(BB)
    BN[...] = jnp.zeros_like(BN)
    TT[...] = jnp.zeros_like(TT)
    l_we.wait()
    l_sn.wait()
    for side in range(2):
        for i in range(3 * BAND):
            f, d = i // BAND, i % BAND
            lo = 0 if i < 8 else 64
            WPK[side, i % 8, :, lo:lo + nz] = WEL[side, f, d]

    wide = 6 * sx
    per = 128 // wide
    for lot in range(0, BAND, per):
        for d in range(lot, min(lot + per, BAND)):
            for side in range(2):
                for f in range(3):
                    at = (d - lot) * wide + (side * 3 + f) * sx
                    TT[at:at + sx, 0:nz] = SNL[side, f, d]
        turned = jnp.transpose(TT[...])[:64]
        for d in range(lot, min(lot + per, BAND)):
            shift = (128 - (d - lot) * wide) % 128
            moved = pltpu.roll(turned, shift, 1) if shift else turned
            BB[:, d, :] = moved
            BN[:, 7 - d, :] = moved
    for q in range(4):
        for side, ref in enumerate((BB, BN)):
            block = jnp.transpose(ref[16 * q:16 * q + 16].reshape(128, 128))
            for f in range(3):
                at = (f * 4 + q) * sx
                SPK[side, at:at + sx, :] = block[(side * 3 + f) * sx:(side * 3 + f + 1) * sx]

    l_r.wait()
    r_all = R[...]
    base = 1.0 + 2.0 * r_all

    def factor(z, prev):
        g = r_all / (base - r_all * prev)
        G[z] = g
        return g

    lax.fori_loop(0, nz, factor, jnp.zeros_like(r_all))

    pl.semaphore_wait(barrier, count)

    def we_copy(side, k):
        dest = 0 if side == 0 else ngx - 1
        return pltpu.make_async_remote_copy(
            src_ref=WPK.at[side], dst_ref=WEB.at[k], send_sem=wssem.at[side],
            recv_sem=wrsem.at[k], device_id=(dest, gy), device_id_type=MESH)

    def sn_rows(part):
        return pl.ds(0, 8 * sx) if part else pl.ds(8 * sx, 4 * sx)

    def sn_copy(side, k, part):
        dest = 0 if side == 0 else ngy - 1
        return pltpu.make_async_remote_copy(
            src_ref=SPK.at[side, sn_rows(part)], dst_ref=SNB.at[k, sn_rows(part)],
            send_sem=sssem.at[side, part], recv_sem=srsem.at[k, part],
            device_id=(gx, dest), device_id_type=MESH)

    for act in ("start", "wait_send"):
        for part in range(2):
            for side in range(2):
                @pl.when(gy != (0 if side == 0 else ngy - 1))
                def _(side=side):
                    getattr(sn_copy(side, gy, part), act)()
    for side in range(2):
        @pl.when(gx != (0 if side == 0 else ngx - 1))
        def _(side=side):
            we_copy(side, gx).start()

    l_rate.wait()
    l_p.wait()
    l_u.wait()
    l_v.wait()

    def rim_tile(f, z, side):
        at = 0 if side == 0 else rx - 8
        if f == 0:
            return U.at[z, 8 + at:16 + at, :]
        if f == 1:
            return V.at[z, at:at + 8, :]
        return PA.at[z, 8 + at:16 + at, :]

    def keep_rim(side):
        def part(i, _):
            for k in range(10):
                for f in range(3):
                    FO[f, i * 10 + k] = rim_tile(f, i * 10 + k, side)[...]
            return 0

        lax.fori_loop(0, nz // 10, part, 0)

    def blend_x(side):
        me = 0 if side == 0 else ngx - 1
        for k in range(ngx):
            if k == me:
                WEB[k] = WPK[side]
            else:
                we_copy(side, k).wait_recv()
        for i in range(8):
            for k in range(ngx):
                TT[k * sy:(k + 1) * sy, :] = WEB[k, i]
            turned = jnp.transpose(TT[...])
            for half in range(2):
                n = i + 8 * half
                if n >= 3 * BAND:
                    continue
                f, d = n // BAND, n % BAND
                QX[f, :, d if side == 0 else 7 - d, :] = turned[64 * half:64 * half + 64]
        at = 0 if side == 0 else rx - 8
        row = lax.broadcasted_iota(jnp.int32, (8, ly), 0).astype(F32)
        dist = row if side == 0 else 7.0 - row
        lane = lax.broadcasted_iota(jnp.int32, (8, ly), 1).astype(F32)
        rate = RW[at:at + 8].astype(F32)
        weight = jnp.maximum(rate - dist, 0.0) / rate
        south = jnp.where(has_s, 0.0, jnp.maximum(rate - lane, 0.0) / rate)
        north = jnp.where(has_n, 0.0, jnp.maximum(rate - ((ly - 1.0) - lane), 0.0) / rate)
        weight = weight * ((1.0 - south) * (1.0 - north))

        def part(i, _):
            for k in range(10):
                for f in range(3):
                    tile = rim_tile(f, i * 10 + k, side)
                    tile[...] = tile[...] + weight * (QX[f, i * 10 + k] - FO[f, i * 10 + k])
            return 0

        lax.fori_loop(0, nz // 10, part, 0)

    def gather_y(side, part):
        me = 0 if side == 0 else ngy - 1
        for k in range(ngy):
            if k == me:
                SNB[k, sn_rows(part)] = SPK[side, sn_rows(part)]
            else:
                sn_copy(side, k, part).wait_recv()
        for k in range(ngy):
            for f in ((0, 1) if part else (2,)):
                for q in range(4):
                    at = (f * 4 + q) * sx
                    QQ[f, q, k * sx:(k + 1) * sx, :] = SNB[k, at:at + sx, :]

    def blend_fields(side, fields, group=None):
        lane = lax.broadcasted_iota(jnp.int32, (rows, ly), 1).astype(F32)
        dist = lane if side == 0 else (ly - 1.0) - lane

        def part(g, _):
            at = pl.multiple_of(g * rows, 8)
            rate = RW[pl.ds(at, rows)].astype(F32)
            weight = jnp.maximum(rate - dist, 0.0) / rate
            for f in fields:
                for z in range(nz):
                    shift = ((0 if side == 0 else 120) + 128 - 8 * (z % 16)) % 128
                    slab = pltpu.roll(QQ[f, z // 16, pl.ds(at, rows)], shift, 1)
                    if f == 0:
                        dst = U.at[z, pl.ds(at + 8, rows), :]
                    elif f == 1:
                        dst = V.at[z, pl.ds(at, rows), :]
                    else:
                        dst = PA.at[z, pl.ds(at + 8, rows), :]
                    old = dst[...]
                    dst[...] = old + weight * (slab - old)
            return 0

        if group is None:
            lax.fori_loop(0, GROUPS, part, 0)
        else:
            part(group, 0)

    QX[...] = jnp.zeros_like(QX)
    for side in range(2):
        @pl.when(gx == (0 if side == 0 else ngx - 1))
        def _(side=side):
            keep_rim(side)
    for side in range(2):
        @pl.when(gy == (0 if side == 0 else ngy - 1))
        def _(side=side):
            gather_y(side, 0)

    pair = lax.broadcasted_iota(jnp.int32, (rows, ly), 1) // 2
    lane_r = lax.broadcasted_iota(jnp.int32, (rows, ly), 1)
    rim = (lane_r == 0) | (lane_r == ly - 1)
    even = lax.rem(lane_r, 2) == 0

    def put(acc, value, z):
        return jnp.where(pair == z, pltpu.roll(value, (2 * z + 1) % 128, 1), acc)

    def own_rows(g):
        return pl.ds(pl.multiple_of(8 + g * rows, 8), rows)

    def all_rows(g):
        return pl.ds(pl.multiple_of(g * rows, 8), rows)

    def in_order(i):
        late = jnp.where(i == GROUPS - 1, 0, jnp.where(i == 0, GROUPS - 1, i))
        both = jnp.where(i == 0, 0, jnp.where(i == 1, GROUPS - 1, i - 1))
        return jnp.where(gx == 0, late, jnp.where(gx == ngx - 1, i, both))

    def put_edges(par, g, acc):
        EB[par, all_rows(g)] = acc
        ES[par, all_rows(g)] = jnp.where(even, pltpu.roll(acc, 127, 1), pltpu.roll(acc, 1, 1))

    def x_west(par):
        return pltpu.make_async_remote_copy(
            src_ref=P[par].at[:, pl.ds(8, 1), :], dst_ref=P[par].at[:, pl.ds(8 + rx, 1), :],
            send_sem=ssem.at[0, par], recv_sem=rsem.at[0, par],
            device_id=(gx - 1, gy), device_id_type=MESH)

    def x_east(par):
        return pltpu.make_async_remote_copy(
            src_ref=P[par].at[:, pl.ds(7 + rx, 1), :], dst_ref=P[par].at[:, pl.ds(7, 1), :],
            send_sem=ssem.at[1, par], recv_sem=rsem.at[1, par],
            device_id=(gx + 1, gy), device_id_type=MESH)

    def u_east():
        return pltpu.make_async_remote_copy(
            src_ref=U.at[:, pl.ds(7 + rx, 1), :], dst_ref=U.at[:, pl.ds(7, 1), :],
            send_sem=ssem.at[10, 0], recv_sem=rsem.at[10, 0],
            device_id=(gx + 1, gy), device_id_type=MESH)

    def y_north(par, g):
        return pltpu.make_async_remote_copy(
            src_ref=ES.at[par, all_rows(g)], dst_ref=RS.at[par, all_rows(g)],
            send_sem=ssem.at[2 + g, par], recv_sem=rsem.at[2 + g, par],
            device_id=(gx, gy + 1), device_id_type=MESH)

    def y_south(par, g):
        return pltpu.make_async_remote_copy(
            src_ref=ES.at[par, all_rows(g)], dst_ref=RN.at[par, all_rows(g)],
            send_sem=ssem.at[6 + g, par], recv_sem=rsem.at[6 + g, par],
            device_id=(gx, gy - 1), device_id_type=MESH)

    def v_north(g):
        return pltpu.make_async_remote_copy(
            src_ref=EV.at[all_rows(g)], dst_ref=RV.at[all_rows(g)],
            send_sem=ssem.at[11 + g, 0], recv_sem=rsem.at[11 + g, 0],
            device_id=(gx, gy + 1), device_id_type=MESH)

    def send_x(par, g):
        @pl.when((g == 0) & has_w)
        def _():
            x_west(par).start()

        @pl.when((g == GROUPS - 1) & has_e)
        def _():
            x_east(par).start()

    def send_y(par, g):
        @pl.when(has_n)
        def _():
            y_north(par, g).start()

        @pl.when(has_s)
        def _():
            y_south(par, g).start()

        @pl.when((g == 0) & jnp.logical_not(has_w))
        def _():
            def part(i, _):
                for k in range(10):
                    P[par][i * 10 + k, 7:8, :] = P[par][i * 10 + k, 8:9, :]
                return 0

            lax.fori_loop(0, nz // 10, part, 0)

    def wait_group(par, g):
        @pl.when((g == 0) & has_w)
        def _():
            x_east(par).wait_recv()
            x_west(par).wait_send()

        @pl.when((g == GROUPS - 1) & has_e)
        def _():
            x_west(par).wait_recv()
            x_east(par).wait_send()

        @pl.when(has_n)
        def _():
            y_south(par, g).wait_recv()
            y_north(par, g).wait_send()

        @pl.when(has_s)
        def _():
            y_north(par, g).wait_recv()
            y_south(par, g).wait_send()

    def s_west():
        return pltpu.make_async_remote_copy(
            src_ref=S.at[:, pl.ds(0, 1), :], dst_ref=S.at[:, pl.ds(rx, 1), :],
            send_sem=ssem.at[10, 1], recv_sem=rsem.at[10, 1],
            device_id=(gx - 1, gy), device_id_type=MESH)

    @pl.when(jnp.logical_not(has_w))
    def _():
        U[:, 7, :] = jnp.zeros((nz, ly), F32)

    @pl.when(jnp.logical_not(has_e))
    def _():
        for par in range(2):
            P[par][:, 8 + rx, :] = jnp.zeros((nz, ly), F32)

    @pl.when(jnp.logical_not(has_n))
    def _():
        RN[...] = jnp.zeros_like(RN)

    @pl.when(jnp.logical_not(has_s))
    def _():
        RV[...] = jnp.zeros_like(RV)

    def first(i, _):
        g = in_order(i)
        send_x(0, g)
        acc = jnp.zeros((rows, ly), F32)
        for z in range(nz):
            acc = put(acc, PA[z, own_rows(g)], z)
        put_edges(0, g, acc)
        send_y(0, g)
        return 0

    def first_v(i, _):
        g = in_order(i)
        acc = jnp.zeros((rows, ly), F32)
        for z in range(nz):
            acc = put(acc, V[z, all_rows(g)], z)
        EV[all_rows(g)] = acc

        @pl.when(has_n)
        def _():
            v_north(g).start()

        return 0

    SN[...] = jnp.zeros_like(SN)

    @pl.when(jnp.logical_not(has_e))
    def _():
        S[:, rx, :] = jnp.zeros((nz, ly), F32)

    first_lane = lane_r == 0
    last_lane = lane_r == ly - 1

    def own_part(p):
        return 0.09 * (4.0 * p - (pltpu.roll(p, 1, 1) + pltpu.roll(p, 127, 1)))

    def ahead(par):
        def part(i, _):
            g = in_order(i)
            for z in range(nz):
                p = P[par][z, own_rows(g)]
                E[z, all_rows(g)] = E[z, all_rows(g)] + own_part(p)
                S[z, all_rows(g)] = S[z, all_rows(g)] + p
            return 0

        lax.fori_loop(0, GROUPS, part, 0)

    def divergence(i, _):
        g = in_order(i)

        @pl.when(has_n)
        def _():
            v_north(g).wait_send()

        @pl.when(has_s)
        def _():
            v_north(g).wait_recv()

        halo_v = RV[all_rows(g)]
        for z in range(nz):
            u = U[z, own_rows(g)]
            uw = U[z, pl.ds(7 + g * rows, rows)]
            v = V[z, all_rows(g)]
            vs = jnp.where(first_lane, pltpu.roll(halo_v, (128 - 2 * z) % 128, 1),
                           pltpu.roll(v, 1, 1))
            p = PA[z, own_rows(g)]
            E[z, all_rows(g)] = 0.3 * ((u - uw) + (v - vs)) + own_part(p)
            S[z, all_rows(g)] = p
        return 0

    def blend_p(i):
        for side in range(2):
            @pl.when(gy == (0 if side == 0 else ngy - 1))
            def _(side=side):
                blend_fields(side, (2,), in_order(i))

    def blend_first(i, _):
        blend_p(i)
        first(i, 0)
        return 0

    at_end = jnp.logical_not(has_w & has_e)
    now = jnp.where(at_end, GROUPS - 1, GROUPS)
    lax.fori_loop(0, now, blend_first, 0)

    @pl.when(at_end)
    def _():
        blend_p(GROUPS - 1)

    for side in range(2):
        @pl.when(gy == (0 if side == 0 else ngy - 1))
        def _(side=side):
            gather_y(side, 1)
            blend_fields(side, (0, 1))

    @pl.when(has_e)
    def _():
        u_east().start()

    lax.fori_loop(0, now, first_v, 0)

    @pl.when(has_e)
    def _():
        u_east().wait_send()

    @pl.when(has_w)
    def _():
        u_east().wait_recv()

    lax.fori_loop(0, now, divergence, 0)
    for side in range(2):
        @pl.when(gx == (0 if side == 0 else ngx - 1))
        def _(side=side):
            blend_x(side)
    for part_of in (first, first_v, divergence):
        lax.fori_loop(now, GROUPS, part_of, 0)

    l_w.wait()

    def corrections(cur, g):
        rn = RN[cur, all_rows(g)]
        rs = jnp.where(has_s, RS[cur, all_rows(g)], EB[cur, all_rows(g)])
        SN[all_rows(g)] = SN[all_rows(g)] + rn
        return jnp.where(even, rn, rs) - ES[cur, all_rows(g)]

    def forward(cur, nxt, g):
        rinv = 1.0 / R[all_rows(g)]
        k_g = corrections(cur, g)

        def get_q(z):
            p = P[cur][z, own_rows(g)]
            pe = P[cur][z, pl.ds(9 + g * rows, rows)]
            pw = P[cur][z, pl.ds(7 + g * rows, rows)]
            k = jnp.where(rim, pltpu.roll(k_g, (255 - 2 * z) % 128, 1), 0.0)
            e = E[z, all_rows(g)] - 0.09 * ((pe + pw) + k)
            E[z, all_rows(g)] = e
            q = p - e
            P[nxt][z, own_rows(g)] = q
            return q

        q, d = get_q(0), jnp.zeros((rows, ly), F32)
        for z in range(nz):
            qn = get_q(z + 1) if z < nz - 1 else None
            diff = q - qn if z < nz - 1 else q
            rhs = W[z, all_rows(g)] + 0.5 * diff
            d = G[z, all_rows(g)] * (rinv * rhs + d)
            W[z, all_rows(g)] = d
            q = qn

    def backward(nxt, g, edges):
        acc = jnp.zeros((rows, ly), F32)
        w = W[nz - 1, all_rows(g)]
        h = 0.5 * w
        for z in range(nz - 2, -2, -1):
            p = P[nxt][z + 1, own_rows(g)] - h
            if z >= 0:
                w = W[z, all_rows(g)] + G[z, all_rows(g)] * w
                W[z, all_rows(g)] = w
                h = 0.5 * w
                p = p + h
            P[nxt][z + 1, own_rows(g)] = p
            if edges:
                acc = put(acc, p, z + 1)
        if edges:
            send_x(nxt, g)
            put_edges(nxt, g, acc)

    def step(cur, nxt, share=False):
        if share:
            @pl.when(has_w)
            def _():
                s_west().start()

        def part(i, _):
            g = in_order(i)
            wait_group(cur, g)
            forward(cur, nxt, g)
            backward(nxt, g, True)
            send_y(nxt, g)
            return 0

        lax.fori_loop(0, GROUPS, part, 0)
        if share:
            @pl.when(has_w)
            def _():
                s_west().wait_send()

        ahead(nxt)

    def two_steps(i, _):
        step(0, 1)
        step(1, 0)
        return 0

    lax.fori_loop(0, (STEPS - 2) // 2, two_steps, 0)
    step(0, 1, share=True)


    def last(i, _):
        g = in_order(i)
        wait_group(1, g)
        forward(1, 0, g)
        backward(0, g, False)
        return 0

    lax.fori_loop(0, GROUPS, last, 0)

    @pl.when(has_e)
    def _():
        s_west().wait_recv()

        def part(i, _):
            for k in range(10):
                z = i * 10 + k
                S[z, rx:rx + 1, :] = S[z, rx:rx + 1, :] + PB[z, 8 + rx:9 + rx, :]
            return 0

        lax.fori_loop(0, nz // 10, part, 0)

    for side in range(2):
        @pl.when(gx != (0 if side == 0 else ngx - 1))
        def _(side=side):
            we_copy(side, gx).wait_send()


def finish(nz, rx, ly, W, PA, U, V, S, SN, uo_hbm, vo_hbm, wo_hbm, po_hbm, UO, VO, osem):
    rows = rx // GROUPS
    store_w = pltpu.make_async_copy(W, wo_hbm, osem.at[0, GROUPS])
    store_p = pltpu.make_async_copy(PA.at[:, pl.ds(8, rx), :], po_hbm, osem.at[1, GROUPS])
    store_w.start()
    store_p.start()
    last_lane = lax.broadcasted_iota(jnp.int32, (rows, ly), 1) == ly - 1

    def store(k, g):
        src, dst = ((UO, uo_hbm), (VO, vo_hbm))[k]
        at = pl.ds(pl.multiple_of(g * rows, 8), rows)
        return pltpu.make_async_copy(src.at[:, at, :], dst.at[:, at, :], osem.at[k, g])

    def winds(g, _):
        at = pl.ds(pl.multiple_of(g * rows, 8), rows)
        halo = SN[at]
        for z in range(nz):
            t = S[z, at]
            te = S[z, pl.ds(g * rows + 1, rows)]
            tn = jnp.where(last_lane, pltpu.roll(halo, (255 - 2 * z) % 128, 1),
                           pltpu.roll(t, 127, 1))
            UO[z, at] = U[z, pl.ds(pl.multiple_of(g * rows + 8, 8), rows)] - 0.3 * (te - t)
            VO[z, at] = V[z, at] - 0.3 * (tn - t)
        store(0, g).start()
        store(1, g).start()
        return 0

    lax.fori_loop(0, GROUPS, winds, 0)
    store_w.wait()
    store_p.wait()
    for g in range(GROUPS):
        store(0, g).wait()
        store(1, g).wait()


def per_device(ngx, ngy, u, v, w, p, r, we, sn, rate):
    nz, rx, ly = p.shape
    we = jnp.transpose(we, (0, 1, 3, 4, 2))
    sn = jnp.transpose(sn, (0, 1, 3, 4, 2))
    field = jax.ShapeDtypeStruct((nz, rx, ly), F32)
    vm = lambda *s: pltpu.VMEM(s, F32)
    hbm = pl.BlockSpec(memory_space=pltpu.HBM)
    vmem = pl.BlockSpec(memory_space=pltpu.VMEM)
    dma = pltpu.SemaphoreType.DMA
    sx = rx // ngy
    scratch = [
        vm(nz, rx + 16, ly), vm(nz, rx, ly), vm(nz, rx, ly),
        vm(rx, ly), pltpu.VMEM((rx, ly), jnp.int32),
        vm(2, 3, BAND, ly // ngx, nz), vm(2, 3, BAND, sx, nz),
        vm(2, 8, ly // ngx, 128), vm(2, 12 * sx, 128),
        vm(ngx, 8, ly // ngx, 128), vm(ngy, 12 * sx, 128),
        vm(128, 128), vm(64, 8, 128), vm(64, 8, 128), vm(3, 4, rx, 128), vm(3, nz, 8, ly),
        vm(3, 64, 8, ly),
        vm(2, rx, ly), vm(2, rx, ly), vm(2, rx, ly), vm(2, rx, ly), vm(rx, ly), vm(rx, ly),
        dma((8,)), dma((11 + GROUPS, 2)), dma((11 + GROUPS, 2)),
        dma((2,)), dma((ngx,)), dma((2, 2)), dma((ngy, 2)),
    ]
    state = pl.pallas_call(
        functools.partial(kernel, ngx, ngy, nz, rx, ly),
        out_shape=(vm(nz, rx, ly), vm(nz, rx + 16, ly), vm(nz, rx + 8, ly), vm(nz, rx, ly),
                   vm(nz, rx + 8, ly), vm(rx, ly)),
        in_specs=[hbm] * 8,
        out_specs=(vmem,) * 6,
        scratch_shapes=scratch,
        compiler_params=pltpu.CompilerParams(collective_id=0, has_side_effects=True,
                                             vmem_limit_bytes=30 * 1024 * 1024),
    )(*(pltpu.with_memory_space_constraint(x, pltpu.HBM) for x in (u, v, w, p, r, we, sn, rate)))
    return pl.pallas_call(
        functools.partial(finish, nz, rx, ly),
        out_shape=(field,) * 4,
        in_specs=[vmem] * 6,
        out_specs=(hbm,) * 4,
        scratch_shapes=[vm(nz, rx, ly), vm(nz, rx, ly), dma((2, GROUPS + 1))],
        compiler_params=pltpu.CompilerParams(vmem_limit_bytes=16 * 1024 * 1024),
    )(*state)


def solution(mesh):
    ngx, ngy = mesh.shape["gx"], mesh.shape["gy"]
    grid = PS(None, "gx", "gy")
    return jax.shard_map(
        functools.partial(per_device, ngx, ngy),
        mesh=mesh,
        in_specs=(grid,) * 4 + (
            PS("gx", "gy"),
            PS(None, None, None, None, ("gy", "gx")),
            PS(None, None, None, None, ("gx", "gy")),
            PS("gx", "gy"),
        ),
        out_specs=(grid,) * 4,
        check_vma=False,
    )
```
